32 devices in a mesh: group: 2 (over x), dp: 2 (over core), tensor: 8 (over z, y).
Axes of the slice: x: 2, y: 2, z: 4, core: 2. Of those that a mesh axis runs over, the one named last changes fastest.
Arguments:
- teacher_hidden: bfloat16 [1024, 8192], P(('group', 'dp'), 'tensor'), may hold values from -6 to 6
- teacher_gain: float32 [8192], P('tensor'), may hold values from 0.1 to 1.9
- project_weight: bfloat16 [8192, 3584], P('tensor'), may hold values from -0.0625 to 0.0625
- student_hidden: bfloat16 [1024, 3584], P(('group', 'dp', 'tensor')), may hold values from -6 to 6
- student_gain: float32 [3584], replicated, may hold values from 0.1 to 1.9
- gate_weight: bfloat16 [3584, 9472], P(('group', 'dp'), 'tensor'), may hold values from -0.09375 to 0.09375
- up_weight: bfloat16 [3584, 9472], P(('group', 'dp'), 'tensor'), may hold values from -0.09375 to 0.09375
- down_weight: bfloat16 [9472, 3584], P('tensor', ('group', 'dp')), may hold values from -0.0625 to 0.0625
- owner_map: int32 [64, 1], P(('group', 'dp')), may hold values from 0 to 3; in each aligned block of 16 rows (0 to 15, 16 to 31, ...) at most 8 rows name the same one
- token_ids: int32 [1024], P(('group', 'dp', 'tensor')), may hold values from 0 to 511
- token_counts: int32 [64], P(('group', 'dp')), may hold values from 1 to 16
- id_weight: float32 [512], replicated, may hold values from 0.25 to 4
Outputs:
- student_out: bfloat16 [4, 16, 32, 3584], P(('group', 'dp'), 'tensor')
- down_grad: float32 [3584, 9472], P(('group', 'dp'), 'tensor')
The draws below stay inside these ranges and needn't reach their ends.
Inputs may be any that keep to these rules, and one draw needn't show every extreme that they name: `owner_map`: of the 16 episodes of one index of group and dp (aligned blocks of 16 rows), at most 8 have the same owner; owner o is index o of group and dp in mesh order.
All inputs are finite; a program needn't handle non-finite values.
Results may differ from the reference program's by a relative error of at most 0.02.
Values may be sent and summed in bfloat16 or wider, within the bound.
A program may use at most 128 MiB of HBM per device.

```python
import math
import jax
import jax.numpy as jnp
import numpy as np
from jax import lax

DT = 8192
DS = 3584
FSW = 9472
REL_VOCAB = 512
EP_LEN = 16
EPI_DEV = 16
SLOTS = 4
EPISODES = 64
TOKENS = 1024
CAP = 8
RECV = 32
N_GROUP = 2
N_DP = 2
N_TENSOR = 8


def set_ends(values, own_key, low, high):
    longest = values.shape.index(max(values.shape))
    spots = []
    for shift in (0, 1):
        where = [jax.random.randint(jax.random.fold_in(own_key, axis), (), 0, length) for axis, length in enumerate(values.shape)]
        where[longest] = (where[longest] + shift) % values.shape[longest]
        spots.append(tuple(where))
    return values.at[spots[0]].set(low).at[spots[1]].set(high)


def level_of(rng, shape, split, least, largest):
    level, own = 1.0, jax.random.fold_in(rng, 6)
    for dim, blocks in split:
        draws = jnp.exp(jax.random.uniform(jax.random.fold_in(own, dim), (blocks,), jnp.float32, least / len(split), largest / len(split)))
        level = level * jnp.repeat(draws, shape[dim] // blocks).reshape([-1 if axis == dim else 1 for axis in range(len(shape))])
    return level


def rank_table(number_of, lean):
    weights = [(1 << 20) // math.isqrt(rank ** lean) + 1 for rank in range(1, number_of + 1)]
    scale = 1 + sum(weights) // (1 << 30)
    return np.cumsum(np.array([max(1, weight // scale) for weight in weights]))


def ranked(key, shape, amount, skew):
    table = rank_table(amount, skew)
    pick = jax.random.randint(jax.random.fold_in(key, 1), shape, 0, int(table[amount - 1]))
    rank = jnp.searchsorted(jnp.asarray(table, jnp.int32), pick, side="right")
    return jax.random.permutation(jax.random.fold_in(key, 2), amount)[rank].astype(jnp.int32)


def assign_block(stream_key, own, number, rows, amount, top, most, skew):
    ranking = jax.random.permutation(stream_key, amount)
    crowded, usual = portions_of(amount, rows * top, most, skew, True), portions_of(amount, rows * top, most, skew, False)
    places = jnp.arange(amount)

    def named(sizes, rotation):
        used = int((sizes > 0).sum())
        fixed = max(1, used // 4)
        passed = fixed + (places - fixed + rotation * (used - fixed)) % max(1, amount - fixed)
        return jnp.zeros((amount,), jnp.int32).at[ranking[jnp.where(places < fixed, places, passed)]].set(jnp.asarray(sizes, jnp.int32))

    sizes = jnp.where(number % 4 == 0, named(crowded, number // 4), named(usual, number - number // 4 - 1))
    mixed = jax.random.permutation(jax.random.fold_in(own, 3), amount)
    donor, taker = mixed[0:amount // 2 * 2:2], mixed[1:amount // 2 * 2:2]
    margin = jnp.minimum(sizes[donor] - 1, most - sizes[taker]) // 2
    margin = jnp.where((donor == ranking[0]) | (taker == ranking[0]) | (sizes[taker] == 0), 0, jnp.maximum(margin, 0))
    passed = jax.random.randint(jax.random.fold_in(own, 4), (amount // 2,), 0, 1 << 20) % (margin + 1)
    sizes = sizes.at[donor].add(-passed).at[taker].add(passed)
    members = jnp.searchsorted(jnp.cumsum(sizes), jnp.arange(rows * top), side="right").astype(jnp.int32)
    grid = members.reshape(top, rows).T
    grid = grid[jax.random.permutation(jax.random.fold_in(own, 1), rows)]
    rotation = jax.random.randint(jax.random.fold_in(own, 2), (rows, 1), 0, top)
    return jnp.take_along_axis(grid, (jnp.arange(top)[None, :] + rotation) % top, axis=1)


def portions_of(amount, total, limit, lean, full):
    weights = [(1 << 20) // math.isqrt(grade ** lean) + 1 for grade in range(1, amount + 1)]
    largest = limit if full else min(limit, max(-(-total // amount), total * weights[0] // sum(weights)))
    least = 1 if total - largest >= amount - 1 else 0
    given, spare = [largest] + [least] * (amount - 1), total - largest - least * (amount - 1)
    while spare > 0:
        movable = [i for i in range(1, amount) if given[i] < largest] or [i for i in range(1, amount) if given[i] < limit]
        pool, remaining = sum([weights[i] for i in movable]), spare
        for i in movable:
            more = min(limit - given[i], max(1, remaining * weights[i] // pool), spare)
            given[i] = given[i] + more
            spare = spare - more
    return np.array(given)


def centred(own_key, shape, spread, reach, cuts=(), held_as=jnp.bfloat16):
    entries = spread * jax.random.normal(own_key, shape, jnp.float32)
    if cuts:
        entries = entries * level_of(own_key, shape, cuts, -0.22, 0.18)
    return jnp.clip(entries, -reach, reach).astype(held_as)


def setup_inputs(seed: int = 0) -> dict:
    streams_of = jax.random.split(jax.random.key(seed), 13)
    teacher_hidden = centred(streams_of[0], (TOKENS, DT), 1.0, 6.0, ((0, 4), (1, 8)))
    teacher_gain = jnp.clip(1.0 + 0.18 * jax.random.normal(streams_of[1], (DT,), jnp.float32), 0.1, 1.9)
    project_weight = centred(streams_of[2], (DT, DS), DT ** -0.5, 0.0625, ((0, 8),))
    student_hidden = centred(streams_of[3], (TOKENS, DS), 1.0, 6.0, ((0, 32),))
    student_gain = jnp.clip(1.0 + 0.18 * jax.random.normal(streams_of[4], (DS,), jnp.float32), 0.1, 1.9)
    gate_weight = centred(streams_of[5], (DS, FSW), DS ** -0.5, 0.09375, ((0, 4), (1, 8)))
    up_weight = centred(streams_of[6], (DS, FSW), DS ** -0.5, 0.09375, ((0, 4), (1, 8)))
    down_weight = centred(streams_of[7], (FSW, DS), FSW ** -0.5, 0.0625, ((0, 8), (1, 4)))
    owner_map_keys = jax.random.split(jax.random.fold_in(streams_of[8], 1), EPISODES // EPI_DEV)
    owner_map_turns = jax.random.permutation(jax.random.fold_in(streams_of[8], 3), EPISODES // EPI_DEV)
    owner_map = jax.vmap(lambda own, number: assign_block(jax.random.fold_in(streams_of[8], 2), own, number, EPI_DEV, SLOTS, 1, CAP, 2))(owner_map_keys, owner_map_turns).reshape((EPISODES, 1))
    token_ids = set_ends(ranked(streams_of[9], (TOKENS,), REL_VOCAB, 2), jax.random.fold_in(streams_of[9], 3), 0, REL_VOCAB - 1).astype(jnp.int32)
    token_counts = set_ends(jax.random.randint(streams_of[10], (EPISODES,), 1, EP_LEN + 1), jax.random.fold_in(streams_of[10], 1), 1, EP_LEN).astype(jnp.int32)
    id_weight = jnp.clip(jnp.exp(jax.random.uniform(streams_of[11], (REL_VOCAB,), jnp.float32, math.log(0.25), math.log(4.0))), 0.25, 4.0)
    return dict(teacher_hidden=teacher_hidden, teacher_gain=teacher_gain, project_weight=project_weight, student_hidden=student_hidden, student_gain=student_gain, gate_weight=gate_weight, up_weight=up_weight, down_weight=down_weight, owner_map=owner_map, token_ids=token_ids, token_counts=token_counts, id_weight=id_weight)


EPSILON = 1e-06

def reference(teacher_hidden, teacher_gain, project_weight, student_hidden, student_gain, gate_weight, up_weight, down_weight, owner_map, token_ids, token_counts, id_weight):
    owners = N_GROUP * N_DP
    token_index = jnp.arange(TOKENS, dtype=jnp.int32)
    position = token_index // EPI_DEV % EP_LEN
    episode = token_index // (EP_LEN * EPI_DEV) * EPI_DEV + token_index % EPI_DEV
    token_weight = jnp.where(position < token_counts[episode], id_weight[token_ids], 0.0).astype(jnp.bfloat16)
    widened = teacher_hidden.astype(jnp.float32)
    inverse = lax.rsqrt(lax.optimization_barrier(jnp.mean(widened * widened, axis=1)) + EPSILON)
    scaled = (widened * teacher_gain[None, :]).astype(jnp.bfloat16)
    feature_block = DT // N_TENSOR

    def add_teacher(index, total):
        offset = (index * feature_block).astype(jnp.int32)
        columns = lax.dynamic_slice_in_dim(scaled, offset, feature_block, 1)
        weight_rows = lax.dynamic_slice_in_dim(project_weight, offset, feature_block, 0)
        partial_sum = jnp.dot(columns, weight_rows, preferred_element_type=jnp.float32).astype(jnp.bfloat16)
        return total + lax.optimization_barrier(partial_sum).astype(jnp.float32)
    summed = lax.fori_loop(0, N_TENSOR, add_teacher, jnp.zeros((TOKENS, DS), jnp.float32))
    projected = (summed * inverse[:, None]).astype(jnp.bfloat16)
    student_wide = student_hidden.astype(jnp.float32)
    rescale = lax.rsqrt(lax.optimization_barrier(jnp.mean(student_wide * student_wide, axis=1, keepdims=True)) + EPSILON)
    normed = (student_wide * rescale * student_gain[None, :]).astype(jnp.bfloat16)
    gate_sum = jnp.dot(normed, gate_weight, preferred_element_type=jnp.float32)
    up_sum = jnp.dot(normed, up_weight, preferred_element_type=jnp.float32)
    activated = (jax.nn.silu(gate_sum) * up_sum).astype(jnp.bfloat16)
    hidden_block = FSW // N_TENSOR

    def add_branch(index, total):
        offset = (index * hidden_block).astype(jnp.int32)
        columns = lax.dynamic_slice_in_dim(activated, offset, hidden_block, 1)
        weight_rows = lax.dynamic_slice_in_dim(down_weight, offset, hidden_block, 0)
        partial_sum = jnp.dot(columns, weight_rows, preferred_element_type=jnp.float32).astype(jnp.bfloat16)
        return total + lax.optimization_barrier(partial_sum).astype(jnp.float32)
    branch = lax.fori_loop(0, N_TENSOR, add_branch, jnp.zeros((TOKENS, DS), jnp.float32))
    predicted = student_wide + branch
    grad_rows = (token_weight.astype(jnp.float32)[:, None] * (predicted - projected.astype(jnp.float32)) / jnp.sqrt(jnp.float32(TOKENS))).astype(jnp.bfloat16)
    owner_list = owner_map[:, 0].reshape(owners, EPI_DEV)
    onehot = (owner_list[:, :, None] == jnp.arange(owners, dtype=jnp.int32)[None, None, :]).astype(jnp.int32)
    earlier = jnp.cumsum(onehot, axis=1) - onehot
    rank_list = lax.optimization_barrier(jnp.sum(earlier * onehot, axis=2))
    target = owner_list * CAP + rank_list
    wanted = jnp.arange(owners, dtype=jnp.int32)[:, None] * CAP + jnp.arange(CAP, dtype=jnp.int32)[None, :]
    matches = (target[None, :, None, :] == wanted[:, None, :, None]).astype(jnp.int32)
    found = lax.optimization_barrier(jnp.sum(matches, axis=3))
    chosen = lax.optimization_barrier(jnp.sum(matches * jnp.arange(EPI_DEV, dtype=jnp.int32)[None, None, None, :], axis=3))
    source_index = jnp.arange(owners, dtype=jnp.int32)[None, None, :, None]
    place_index = jnp.arange(EP_LEN, dtype=jnp.int32)[None, :, None, None]
    row_index = (source_index * EP_LEN + place_index) * EPI_DEV + chosen[:, None, :, :]
    row_index = jnp.where(found[:, None, :, :] > 0, row_index, TOKENS).astype(jnp.int32)
    row_index = row_index.reshape(owners, EP_LEN * owners * CAP)
    padded_out = jnp.concatenate([predicted.astype(jnp.bfloat16), jnp.zeros((1, DS), jnp.bfloat16)], axis=0)
    student_out = jnp.take(padded_out, row_index.reshape(-1), axis=0).reshape(owners, EP_LEN, RECV, DS)
    grad_padded = jnp.concatenate([grad_rows, jnp.zeros((1, DS), jnp.bfloat16)], axis=0)
    act_padded = jnp.concatenate([activated, jnp.zeros((1, FSW), jnp.bfloat16)], axis=0)

    def add_owner(index, total):
        chosen_rows = row_index[index]
        grad_part = jnp.take(grad_padded, chosen_rows, axis=0).astype(jnp.float32)
        act_part = jnp.take(act_padded, chosen_rows, axis=0).astype(jnp.float32)
        term = jnp.einsum('rc,rh->ch', grad_part, act_part)
        return total + lax.optimization_barrier(term.astype(jnp.bfloat16)).astype(jnp.float32)
    down_grad = lax.fori_loop(0, owners, add_owner, jnp.zeros((DS, FSW), jnp.float32))
    return (student_out, down_grad)
```

```python
import functools
import math

import jax
import jax.numpy as jnp
from jax import lax
from jax.experimental import pallas as pl
from jax.experimental.pallas import tpu as pltpu
from jax.sharding import PartitionSpec as P

EP_LEN = 16
EXTRA = 128
EPSILON = 1e-06
OWNER_AXES = ("group", "dp")


def exchange(blocks):
    return lax.all_to_all(blocks, OWNER_AXES, split_axis=0, concat_axis=0, tiled=True)


def by_columns(rows, owners):
    return rows.reshape(rows.shape[0], owners, -1).transpose(1, 0, 2)


def three_terms(values):
    high = lax.reduce_precision(values, 8, 7)
    rest = values - high
    middle = lax.reduce_precision(rest, 8, 7)
    return high, middle, rest - middle


def build_selector(owner_list, owners, capacity):
    onehot = (owner_list[:, :, None] == jnp.arange(owners, dtype=jnp.int32)).astype(jnp.int32)
    earlier = jnp.cumsum(onehot, axis=1) - onehot
    rank_list = jnp.sum(earlier * onehot, axis=2)
    target = owner_list * capacity + rank_list
    slots = jnp.arange(owners * capacity, dtype=jnp.int32)
    return (target[:, None, :] == slots[None, :, None]).astype(jnp.bfloat16)


def general(
    teacher_hidden,
    teacher_gain,
    project_weight,
    student_hidden,
    student_gain,
    gate_weight,
    up_weight,
    down_weight,
    owner_map,
    token_ids,
    token_counts,
    id_weight,
):
    owners = lax.axis_size("group") * lax.axis_size("dp")
    tensors = lax.axis_size("tensor")
    tensor_index = lax.axis_index("tensor")
    owner_index = lax.axis_index(OWNER_AXES)
    episodes = token_counts.shape[0]
    own_span = EP_LEN // tensors
    share = own_span * episodes
    capacity = max(2, 2 * episodes // owners)
    received = owners * capacity
    student_width = student_hidden.shape[1]
    width = student_width // owners
    tokens_all = EP_LEN * episodes * owners
    teacher_width = teacher_hidden.shape[1] * tensors

    id_rows = token_ids.reshape(own_span, episodes)
    looked = jnp.sum(
        jnp.where(
            id_rows[:, :, None] == jnp.arange(id_weight.shape[0], dtype=jnp.int32)[None, None, :],
            id_weight[None, None, :],
            0.0,
        ),
        axis=2,
    )
    position = tensor_index * own_span + jnp.arange(own_span, dtype=jnp.int32)[:, None]
    token_weight = jnp.where(position < token_counts[None, :], looked, 0.0).reshape(share, 1)

    own_rows = student_hidden.astype(jnp.float32)
    own_rescale = lax.rsqrt(jnp.mean(own_rows * own_rows, axis=1, keepdims=True) + EPSILON)
    owner_rows = jnp.tile(owner_map.astype(jnp.float32), (own_span, 1))
    extras = jnp.concatenate([token_weight, owner_rows, *three_terms(own_rescale)], axis=1)
    extras = jnp.pad(extras, ((0, 0), (0, EXTRA - extras.shape[1]))).astype(jnp.bfloat16)
    arrived = exchange(
        jnp.concatenate(
            [
                by_columns(student_hidden, owners),
                jnp.broadcast_to(extras[None], (owners, share, EXTRA)),
            ],
            axis=2,
        )
    )
    rows = owners * share
    student_block = arrived[:, :, :width].reshape(rows, width).astype(jnp.float32)
    facts = arrived[:, :, width:].astype(jnp.float32)
    weight_rows = facts[:, :, 0].reshape(rows, 1)
    owner_list = facts[:, :episodes, 1].astype(jnp.int32)
    rescale = (facts[:, :, 2] + facts[:, :, 3] + facts[:, :, 4]).reshape(rows, 1)
    gain = lax.dynamic_slice_in_dim(student_gain, owner_index * width, width, 0)
    normed = (student_block * rescale * gain[None, :]).astype(jnp.bfloat16)
    gathered = lax.all_gather(normed, "tensor", axis=0, tiled=True)

    widened = teacher_hidden.astype(jnp.float32)
    squares = jnp.sum(widened * widened, axis=1)
    scaled = (widened * teacher_gain[None, :]).astype(jnp.bfloat16)
    inverse = lax.rsqrt(lax.psum(squares, "tensor") / teacher_width + EPSILON)
    summed = lax.psum_scatter(
        jnp.dot(scaled, project_weight, preferred_element_type=jnp.float32).astype(jnp.bfloat16),
        "tensor",
        scatter_dimension=0,
        tiled=True,
    ).astype(jnp.float32)
    own_inverse = lax.dynamic_slice_in_dim(inverse, tensor_index * share, share, 0)
    projected = exchange(by_columns((summed * own_inverse[:, None]).astype(jnp.bfloat16), owners))

    hidden = gate_weight.shape[1]
    gate_part = jnp.dot(gathered, gate_weight, preferred_element_type=jnp.float32)
    up_part = jnp.dot(gathered, up_weight, preferred_element_type=jnp.float32)
    parts = jnp.stack(
        [
            gate_part.astype(jnp.bfloat16).reshape(owners, -1, hidden),
            up_part.astype(jnp.bfloat16).reshape(owners, -1, hidden),
        ],
        axis=1,
    )
    sums = lax.psum_scatter(parts, OWNER_AXES, scatter_dimension=0, tiled=True).astype(jnp.float32)
    activated = (jax.nn.silu(sums[0, 0]) * sums[0, 1]).astype(jnp.bfloat16)
    act_all = lax.all_gather(activated, OWNER_AXES, axis=0, tiled=True)
    branch = jnp.dot(act_all, down_weight, preferred_element_type=jnp.float32)
    branch_local = lax.psum_scatter(
        branch.astype(jnp.bfloat16), "tensor", scatter_dimension=0, tiled=True
    ).astype(jnp.float32)
    predicted = student_block + branch_local

    difference = predicted - projected.reshape(rows, width).astype(jnp.float32)
    grad_block = (weight_rows * difference * (1.0 / math.sqrt(tokens_all))).astype(jnp.bfloat16)
    grad_all = lax.all_gather(grad_block, "tensor", axis=0, tiled=True)
    down_grad = jnp.einsum("rc,rh->ch", grad_all, act_all, preferred_element_type=jnp.float32)

    selector = build_selector(owner_list, owners, capacity)
    picked = jnp.einsum(
        "sre,spef->sprf",
        selector,
        predicted.astype(jnp.bfloat16).reshape(owners, own_span, episodes, width),
        preferred_element_type=jnp.float32,
    ).astype(jnp.bfloat16)
    outgoing = picked.reshape(owners, own_span, owners, capacity, width).transpose(2, 1, 0, 3, 4)
    incoming = exchange(outgoing.reshape(owners, own_span, received, width))
    student_out = incoming.transpose(1, 2, 0, 3).reshape(1, own_span, received, student_width)
    return (student_out, down_grad)


MESH = pl.DeviceIdType.MESH
TILE = 256


def over_tiles(width, body):
    whole = width // TILE

    def step(index, carry):
        body(pl.multiple_of(index * TILE, TILE), TILE)
        return carry

    if whole:
        lax.fori_loop(0, whole, step, 0)
    if width > whole * TILE:
        body(whole * TILE, width - whole * TILE)


def column_of(row, eye):
    return jnp.sum(jnp.where(eye, row, 0.0), axis=1, keepdims=True)


def fused_kernel(
    size,
    teacher_ref,
    teacher_gain_ref,
    project_ref,
    student_ref,
    student_gain_ref,
    gate_ref,
    up_ref,
    down_ref,
    owner_ref,
    ids_ref,
    counts_ref,
    id_weight_ref,
    grad_out,
    act_out,
    student_out,
    th,
    scaled,
    pw,
    tp,
    st,
    nrm,
    gw,
    uw,
    dw,
    nb,
    own_part,
    d2s,
    d2r,
    own_x,
    xs,
    xr,
    act,
    bp0,
    rss,
    rsr,
    trs,
    trr,
    sqs,
    sqr,
    inverse_ref,
    pjs,
    pj,
    sb,
    ext,
    ga,
    predb,
    sos,
    so,
    load_sem,
    nx_s,
    nx_r,
    raw_s,
    raw_r,
    ext_s,
    ext_r,
    pj_s,
    pj_r,
    so_s,
    so_r,
    sq_s,
    sq_r,
    ag_s,
    ag_r,
    tr_s,
    tr_r,
    rs_s,
    rs_r,
    gg_s,
    gg_r,
    d2_s,
    d2_r,
    x_s,
    x_r,
    a1_s,
    a1_r,
    a2_s,
    a2_r,
    a3_s,
    a3_r,
    out_sem,
):
    T, O, E, span, cap = size["T"], size["O"], size["E"], size["span"], size["cap"]
    share = span * E
    rows = O * share
    half, quarter = rows // 2, rows // 4
    W = nb.shape[2]
    H = gw.shape[1]
    DS = st.shape[1]
    t_half = share // 2
    f32, bf16 = jnp.float32, jnp.bfloat16

    x = lax.axis_index("group")
    c = lax.axis_index("dp")
    t = lax.axis_index("tensor")
    o = x * 2 + c
    odd = lax.rem(t, 2)
    r = (1 - odd) * lax.div(t, 2) + odd * (T - 1 - lax.div(t, 2))

    def at_ring(position):
        p = lax.rem(position, T)
        upper = lax.div(p, T // 2)
        return (1 - upper) * (2 * p) + upper * (2 * (T - 1 - p) + 1)

    nxt, prv = at_ring(r + 1), at_ring(r + T - 1)
    peers = (
        (1 - x, c, {"group": 1 - x}),
        (1 - x, 1 - c, {"group": 1 - x, "dp": 1 - c}),
        (x, 1 - c, {"dp": 1 - c}),
    )
    other_chip, core_peer = {"group": 1 - x}, {"dp": 1 - c}

    def remote(src, dst, send, recv, device):
        return pltpu.make_async_remote_copy(
            src_ref=src, dst_ref=dst, send_sem=send, recv_sem=recv, device_id=device, device_id_type=MESH
        )

    loads = [
        pltpu.make_async_copy(src, dst, load_sem.at[index])
        for index, (src, dst) in enumerate(
            [(student_ref, st), (teacher_ref, th), (project_ref, pw), (gate_ref, gw), (up_ref, uw), (down_ref, dw)]
        )
    ]
    for load in loads:
        load.start()

    barrier = pltpu.get_barrier_semaphore()
    for _, _, device in peers:
        pl.semaphore_signal(barrier, inc=1, device_id=device, device_id_type=MESH)
    for step in range(1, T):
        pl.semaphore_signal(barrier, inc=1, device_id={"tensor": at_ring(r + step)}, device_id_type=MESH)

    def columns(owner):
        return pl.ds(pl.multiple_of(owner * W, W), W)

    def owner_rows(owner):
        return pl.ds(pl.multiple_of(owner * share, share), share)

    def nx(k):
        return remote(
            nrm.at[:, columns(peers[k][0] * 2 + peers[k][1])],
            nb.at[0, owner_rows(o), :],
            nx_s.at[k],
            nx_r.at[k],
            peers[k][2],
        )

    def raw(k):
        return remote(
            st.at[:, columns(peers[k][0] * 2 + peers[k][1])],
            sb.at[owner_rows(o), :],
            raw_s.at[k],
            raw_r.at[k],
            peers[k][2],
        )

    def extra(k):
        return remote(ext.at[o], ext.at[o], ext_s.at[k], ext_r.at[k], peers[k][2])

    def proj(k):
        return remote(
            pjs.at[:, columns(peers[k][0] * 2 + peers[k][1])],
            pj.at[owner_rows(o), :],
            pj_s.at[k],
            pj_r.at[k],
            peers[k][2],
        )

    out_rows = span * O * cap

    def outgoing(k):
        q = peers[k][0] * 2 + peers[k][1]
        return remote(
            sos.at[pl.ds(pl.multiple_of(q * out_rows, out_rows), out_rows), :],
            so.at[:, columns(o)],
            so_s.at[k],
            so_r.at[k],
            peers[k][2],
        )

    def block_rows(position):
        return pl.ds(pl.multiple_of(at_ring(position) * share, share), share)

    def squares(step):
        return remote(
            sqs.at[block_rows(r + step), :],
            sqr.at[step],
            sq_s.at[step],
            sq_r.at[step],
            {"tensor": at_ring(r + step)},
        )

    def to(d):
        return {"tensor": nxt if d == 0 else prv}

    def part(d, n):
        return pl.ds(d * n, n)

    def ag(d, g):
        return remote(
            nb.at[g - 1, part(d, half), :], nb.at[g, part(d, half), :], ag_s.at[d, g], ag_r.at[d, g], to(d)
        )

    def rs(d, g):
        return remote(
            rss.at[g, part(d, half), :], rsr.at[g, part(d, half), :], rs_s.at[d, g], rs_r.at[d, g], to(d)
        )

    def tr(d, k):
        return remote(
            trs.at[k, part(d, t_half), :], trr.at[k, part(d, t_half), :], tr_s.at[d, k], tr_r.at[d, k], to(d)
        )

    def gg(s, g):
        d = s * 2 // O
        return remote(
            ga.at[g - 1, part(s, share), :], ga.at[g, part(s, share), :], gg_s.at[s, g], gg_r.at[s, g], to(d)
        )

    def d2(g):
        return remote(d2s.at[g], d2r.at[g], d2_s.at[g], d2_r.at[g], core_peer)

    def xch(g):
        return remote(xs.at[g], xr.at[g], x_s.at[g], x_r.at[g], other_chip)

    def act_rows(core, chip):
        return pl.ds(pl.multiple_of((core * 2 + chip) * quarter, quarter), quarter)

    own_act = act_rows(c, x)
    far_act = act_rows(c, 1 - x)

    def a1(g):
        return remote(act.at[g, own_act, :], act.at[g, own_act, :], a1_s.at[g], a1_r.at[g], other_chip)

    def a2(g):
        return remote(act.at[g, own_act, :], act.at[g, own_act, :], a2_s.at[g], a2_r.at[g], core_peer)

    def a3(g):
        return remote(act.at[g, far_act, :], act.at[g, far_act, :], a3_s.at[g], a3_r.at[g], core_peer)

    loads[0].wait()
    wide = st[...].astype(f32)
    rescale = lax.rsqrt(jnp.mean(wide * wide, axis=1, keepdims=True) + EPSILON)
    nrm[...] = (wide * rescale * student_gain_ref[...]).astype(bf16)
    pl.semaphore_wait(barrier, len(peers) + T - 1)
    for k in range(len(peers)):
        nx(k).start()
    nb[0, owner_rows(o), :] = nrm[:, columns(o)]
    sb[owner_rows(o), :] = st[:, columns(o)]

    def iota(shape, axis):
        return lax.broadcasted_iota(jnp.int32, shape, axis)

    ids = ids_ref[...].astype(f32)
    ids_column = column_of(ids, iota((share, share), 0) == iota((share, share), 1))
    vocabulary = id_weight_ref.shape[1]
    looked = jnp.sum(
        jnp.where(ids_column == iota((share, vocabulary), 1).astype(f32), id_weight_ref[...], 0.0),
        axis=1,
        keepdims=True,
    )
    row_of = iota((share, E), 0)
    counts = column_of(counts_ref[...].astype(f32), lax.rem(row_of, E) == iota((share, E), 1))
    place = (t * span + lax.div(iota((share, 1), 0), E)).astype(f32)
    token_weight = jnp.where(place < counts, looked, 0.0).astype(bf16).astype(f32)
    own_column = owner_ref[...].astype(f32)
    episode_row, episode_lane = iota((E, 128), 0), lax.rem(iota((E, 128), 1), E)
    own_lane = jnp.sum(jnp.where(episode_row == episode_lane, own_column, 0.0), axis=0, keepdims=True)
    rank = jnp.sum(
        jnp.where((own_column == own_lane) & (episode_row < episode_lane), 1.0, 0.0), axis=0, keepdims=True
    )
    target = own_lane * cap + rank
    ext[o, 0:share, :] = jnp.broadcast_to(token_weight, (share, 128))
    ext[o, share : share + 8, :] = jnp.broadcast_to(target, (8, 128))
    for k in range(len(peers)):
        raw(k).start()
        extra(k).start()

    loads[1].wait()
    wide = th[...].astype(f32)
    scaled[...] = (wide * teacher_gain_ref[...]).astype(bf16)
    sqs[...] = jnp.broadcast_to(jnp.sum(wide * wide, axis=1, keepdims=True), sqs.shape)
    for step in range(1, T):
        squares(step).start()
    loads[2].wait()

    def teacher_tile(offset, n):
        tp[:, pl.ds(offset, n)] = jnp.dot(
            scaled[...], pw[:, pl.ds(offset, n)], preferred_element_type=f32
        ).astype(bf16)

    over_tiles(DS, teacher_tile)
    trr[0] = jnp.zeros(trr.shape[1:], bf16)
    rsr[0] = jnp.zeros(rsr.shape[1:], bf16)

    def teacher_rows(position, d):
        return pl.ds(pl.multiple_of(at_ring(position) * share + d * t_half, t_half), t_half)

    def teacher_step(k):
        @pl.when(k > 1)
        def _():
            tr(0, k - 1).wait_recv()
            tr(1, k - 1).wait_recv()

        for d in (0, 1):
            position = r + T - k if d == 0 else r + k
            trs[k, part(d, t_half), :] = (
                tp[teacher_rows(position, d), :].astype(f32) + trr[k - 1, part(d, t_half), :].astype(f32)
            ).astype(bf16)
            tr(d, k).start()

    for k in range(len(peers)):
        nx(k).wait_recv()
    loads[3].wait()
    loads[4].wait()
    loads[5].wait()

    def p1(g):
        @pl.when(g > 0)
        def _():
            ag(0, g).wait_recv()
            ag(1, g).wait_recv()

        @pl.when(g < T - 1)
        def _():
            ag(0, g + 1).start()
            ag(1, g + 1).start()

        away = pl.ds(pl.multiple_of((1 - c) * half, half), half)
        here = pl.ds(pl.multiple_of(c * half, half), half)
        for m, weight in enumerate((gw, uw)):

            def tile(offset, n):
                lhs = jnp.concatenate([nb[g, away, :], nb[g, here, :]], axis=0)
                value = jnp.dot(lhs, weight[:, pl.ds(offset, n)], preferred_element_type=f32)
                d2s[g, m, :, pl.ds(offset, n)] = value[:half].astype(bf16)
                own_part[m, :, pl.ds(offset, n)] = value[half:]

            over_tiles(H, tile)
        d2(g).start()

    def p2(g):
        d2(g).wait_recv()
        far = pl.ds(pl.multiple_of((1 - x) * quarter, quarter), quarter)
        near = pl.ds(pl.multiple_of(x * quarter, quarter), quarter)
        for m in (0, 1):
            xs[g, m] = (own_part[m, far, :] + d2r[g, m, far, :].astype(f32)).astype(bf16)
        xch(g).start()
        for m in (0, 1):
            own_x[m] = own_part[m, near, :] + d2r[g, m, near, :].astype(f32)

    def p3(g):
        xch(g).wait_recv()
        gate = own_x[0] + xr[g, 0].astype(f32)
        up = own_x[1] + xr[g, 1].astype(f32)
        act[g, own_act, :] = (gate / (1.0 + jnp.exp(-gate)) * up).astype(bf16)
        a1(g).start()
        a2(g).start()

    def p4(g):
        a1(g).wait_recv()
        a3(g).start()

    def act_store(g):
        return pltpu.make_async_copy(act.at[g], act_out.at[g], out_sem.at[0, g])

    def p5(g):
        a2(g).wait_recv()
        a3(g).wait_recv()
        act_store(g).start()

        @pl.when(g > 1)
        def _():
            rs(0, g - 1).wait_recv()
            rs(1, g - 1).wait_recv()

        def tile(offset, n):
            value = jnp.dot(act[g], dw[:, pl.ds(offset, n)], preferred_element_type=f32)

            @pl.when(g == 0)
            def _():
                bp0[:, pl.ds(offset, n)] = value

            @pl.when(g > 0)
            def _():
                rss[g, :, pl.ds(offset, n)] = (
                    value + rsr[jnp.maximum(g - 1, 0), :, pl.ds(offset, n)].astype(f32)
                ).astype(bf16)

        over_tiles(W, tile)

        @pl.when(g > 0)
        def _():
            rs(0, g).start()
            rs(1, g).start()

    def finish_teacher():
        tr(0, T - 1).wait_recv()
        tr(1, T - 1).wait_recv()
        total = sqs[block_rows(r), :]
        for step in range(1, T):
            squares(step).wait_recv()
            total = total + sqr[step]
        inverse_ref[...] = lax.rsqrt(total * (1.0 / size["teacher_width"]) + EPSILON)
        for d in (0, 1):
            summed = tp[teacher_rows(r, d), :].astype(f32) + trr[T - 1, part(d, t_half), :].astype(f32)
            pjs[part(d, t_half), :] = (summed * inverse_ref[part(d, t_half), 0:1]).astype(bf16)
        for k in range(len(peers)):
            proj(k).start()
        pj[owner_rows(o), :] = pjs[:, columns(o)]

    def step(i, carry):
        @pl.when(i < T)
        def _():
            p1(i)

        @pl.when(i < T - 1)
        def _():
            teacher_step(i + 1)

        @pl.when(i == T - 1)
        def _():
            finish_teacher()

        @pl.when(i >= 2)
        def _():
            p4(i - 2)
            p5(i - 2)

        @pl.when((i >= 1) & (i <= T))
        def _():
            p3(i - 1)

        @pl.when(i < T)
        def _():
            p2(i)

        return carry

    lax.fori_loop(0, T + 2, step, 0)

    for k in range(len(peers)):
        raw(k).wait_recv()
        extra(k).wait_recv()
        proj(k).wait_recv()
    rs(0, T - 1).wait_recv()
    rs(1, T - 1).wait_recv()
    order = [s for pair in zip(range(O // 2), range(O // 2, O)) for s in pair]
    for s in order:
        own = slice(s * share, (s + 1) * share)
        predicted = sb[own, :].astype(f32) + (bp0[own, :] + rsr[T - 1, own, :].astype(f32))
        predb[own, :] = predicted.astype(bf16)
        difference = predicted - pj[own, :].astype(f32)
        ga[0, own, :] = (ext[s, 0:share, 0:1] * difference * size["scale"]).astype(bf16)
        gg(s, 1).start()

    def grad_store(g):
        return pltpu.make_async_copy(ga.at[g], grad_out.at[g], out_sem.at[1, g])

    grad_store(0).start()

    lane = iota((1, rows), 1)
    wanted_target = jnp.zeros((1, rows), f32)
    for s in range(O):
        wanted_target = jnp.where(lax.div(lane, share) == s, ext[s, share : share + 1, :], wanted_target)
    picks = O * out_rows
    line = iota((picks, rows), 0)
    place_row = lax.rem(lax.div(line, O * cap), span)
    source_row = lax.rem(lax.div(line, cap), O)
    slot = (lax.div(line, out_rows) * cap + lax.rem(line, cap)).astype(f32)
    lanes = iota((picks, rows), 1)
    chosen = (
        (wanted_target == slot)
        & (lax.div(lanes, share) == source_row)
        & (lax.div(lax.rem(lanes, share), E) == place_row)
    )
    selector = jnp.where(chosen, 1.0, 0.0).astype(bf16)

    def pick_tile(offset, n):
        sos[:, pl.ds(offset, n)] = jnp.dot(
            selector, predb[:, pl.ds(offset, n)], preferred_element_type=f32
        ).astype(bf16)

    over_tiles(W, pick_tile)
    for k in range(len(peers)):
        outgoing(k).start()
    so[:, columns(o)] = sos[pl.ds(pl.multiple_of(o * out_rows, out_rows), out_rows), :]

    def gather_step(g, carry):
        for s in order:
            gg(s, g).wait_recv()

            @pl.when(g < T - 1)
            def _():
                gg(s, g + 1).start()

        grad_store(g).start()
        return carry

    lax.fori_loop(1, T, gather_step, 0)

    for k in range(len(peers)):
        outgoing(k).wait_recv()
    student_store = pltpu.make_async_copy(so, student_out, out_sem.at[0, T])
    student_store.start()

    def drain(g, carry):
        for copy in (d2, xch, a1, a2, a3):
            copy(g).wait_send()
        act_store(g).wait()
        grad_store(g).wait()

        @pl.when(g > 0)
        def _():
            squares(g).wait_send()
            for d in (0, 1):
                ag(d, g).wait_send()
                rs(d, g).wait_send()
                tr(d, g).wait_send()
            for s in range(O):
                gg(s, g).wait_send()

        return carry

    lax.fori_loop(0, T, drain, 0)
    for k in range(len(peers)):
        nx(k).wait_send()
        raw(k).wait_send()
        extra(k).wait_send()
        proj(k).wait_send()
        outgoing(k).wait_send()
    student_store.wait()


def fused(
    teacher_hidden,
    teacher_gain,
    project_weight,
    student_hidden,
    student_gain,
    gate_weight,
    up_weight,
    down_weight,
    owner_map,
    token_ids,
    token_counts,
    id_weight,
):
    f32, bf16 = jnp.float32, jnp.bfloat16
    T, O = lax.axis_size("tensor"), lax.axis_size("group") * lax.axis_size("dp")
    E = token_counts.shape[0]
    span = EP_LEN // T
    share = span * E
    rows = O * share
    half, quarter = rows // 2, rows // 4
    cap = max(2, 2 * E // O)
    local_tokens, F = teacher_hidden.shape
    DS = student_hidden.shape[1]
    W, H = gate_weight.shape
    out_rows = span * O * cap
    size = dict(
        T=T,
        O=O,
        E=E,
        span=span,
        cap=cap,
        teacher_width=F * T,
        scale=1.0 / math.sqrt(EP_LEN * E * O),
    )
    vmem = pl.BlockSpec(memory_space=pltpu.VMEM)
    anywhere = pl.BlockSpec(memory_space=pl.ANY)
    DMA = pltpu.SemaphoreType.DMA
    scratch = [
        pltpu.VMEM((local_tokens, F), bf16),
        pltpu.VMEM((local_tokens, F), bf16),
        pltpu.VMEM((F, DS), bf16),
        pltpu.VMEM((local_tokens, DS), bf16),
        pltpu.VMEM((share, DS), bf16),
        pltpu.VMEM((share, DS), bf16),
        pltpu.VMEM((W, H), bf16),
        pltpu.VMEM((W, H), bf16),
        pltpu.VMEM((H, W), bf16),
        pltpu.VMEM((T, rows, W), bf16),
        pltpu.VMEM((2, half, H), f32),
        pltpu.VMEM((T, 2, half, H), bf16),
        pltpu.VMEM((T, 2, half, H), bf16),
        pltpu.VMEM((2, quarter, H), f32),
        pltpu.VMEM((T, 2, quarter, H), bf16),
        pltpu.VMEM((T, 2, quarter, H), bf16),
        pltpu.VMEM((T, rows, H), bf16),
        pltpu.VMEM((rows, W), f32),
        pltpu.VMEM((T, rows, W), bf16),
        pltpu.VMEM((T, rows, W), bf16),
        pltpu.VMEM((T, share, DS), bf16),
        pltpu.VMEM((T, share, DS), bf16),
        pltpu.VMEM((local_tokens, 128), f32),
        pltpu.VMEM((T, share, 128), f32),
        pltpu.VMEM((share, 128), f32),
        pltpu.VMEM((share, DS), bf16),
        pltpu.VMEM((rows, W), bf16),
        pltpu.VMEM((rows, W), bf16),
        pltpu.VMEM((O, share + 8, 128), f32),
        pltpu.VMEM((T, rows, W), bf16),
        pltpu.VMEM((rows, W), bf16),
        pltpu.VMEM((O * out_rows, W), bf16),
        pltpu.VMEM((out_rows, DS), bf16),
        DMA((6,)),
        *[DMA((3,)) for _ in range(10)],
        *[DMA((T,)) for _ in range(2)],
        *[DMA((2, T)) for _ in range(6)],
        *[DMA((O, T)) for _ in range(2)],
        *[DMA((T,)) for _ in range(10)],
        DMA((2, T + 1)),
    ]
    grads, acts, out = pl.pallas_call(
        functools.partial(fused_kernel, size),
        out_shape=(
            jax.ShapeDtypeStruct((T, rows, W), bf16),
            jax.ShapeDtypeStruct((T, rows, H), bf16),
            jax.ShapeDtypeStruct((out_rows, DS), bf16),
        ),
        in_specs=[anywhere, vmem, anywhere, anywhere, vmem, anywhere, anywhere, anywhere, vmem, vmem, vmem, vmem],
        out_specs=(anywhere, anywhere, anywhere),
        scratch_shapes=scratch,
        compiler_params=pltpu.CompilerParams(
            collective_id=0, has_side_effects=True, vmem_limit_bytes=63 * 1024 * 1024
        ),
    )(
        teacher_hidden,
        teacher_gain.reshape(1, F),
        project_weight,
        student_hidden,
        student_gain.reshape(1, DS),
        gate_weight,
        up_weight,
        down_weight,
        owner_map,
        token_ids.reshape(1, share),
        token_counts.reshape(1, E),
        id_weight.reshape(1, -1),
    )
    down_grad = jnp.einsum(
        "rc,rh->ch", grads.reshape(T * rows, W), acts.reshape(T * rows, H), preferred_element_type=f32
    )
    return (out.reshape(1, span, O * cap, DS), down_grad)


def fits(mesh):
    return mesh.shape["group"] == 2 and mesh.shape["dp"] == 2 and mesh.shape["tensor"] == 8


def solution(mesh):
    in_specs = (
        P(("group", "dp"), "tensor"),
        P("tensor"),
        P("tensor", None),
        P(("group", "dp", "tensor"), None),
        P(),
        P(("group", "dp"), "tensor"),
        P(("group", "dp"), "tensor"),
        P("tensor", ("group", "dp")),
        P(("group", "dp"), None),
        P(("group", "dp", "tensor")),
        P(("group", "dp")),
        P(),
    )
    out_specs = (P(("group", "dp"), "tensor", None, None), P(("group", "dp"), "tensor"))
    body = fused if fits(mesh) else general
    return jax.shard_map(body, mesh=mesh, in_specs=in_specs, out_specs=out_specs, check_vma=False)
```

```python
import functools
import math

import jax
import jax.numpy as jnp
from jax import lax
from jax.experimental import pallas as pl
from jax.experimental.pallas import tpu as pltpu
from jax.sharding import PartitionSpec as P

EP_LEN = 16
EXTRA = 128
EPSILON = 1e-06
OWNER_AXES = ("group", "dp")


def exchange(blocks):
    return lax.all_to_all(blocks, OWNER_AXES, split_axis=0, concat_axis=0, tiled=True)


def by_columns(rows, owners):
    return rows.reshape(rows.shape[0], owners, -1).transpose(1, 0, 2)


def three_terms(values):
    high = lax.reduce_precision(values, 8, 7)
    rest = values - high
    middle = lax.reduce_precision(rest, 8, 7)
    return high, middle, rest - middle


def build_selector(owner_list, owners, capacity):
    onehot = (owner_list[:, :, None] == jnp.arange(owners, dtype=jnp.int32)).astype(jnp.int32)
    earlier = jnp.cumsum(onehot, axis=1) - onehot
    rank_list = jnp.sum(earlier * onehot, axis=2)
    target = owner_list * capacity + rank_list
    slots = jnp.arange(owners * capacity, dtype=jnp.int32)
    return (target[:, None, :] == slots[None, :, None]).astype(jnp.bfloat16)


def general(
    teacher_hidden,
    teacher_gain,
    project_weight,
    student_hidden,
    student_gain,
    gate_weight,
    up_weight,
    down_weight,
    owner_map,
    token_ids,
    token_counts,
    id_weight,
):
    owners = lax.axis_size("group") * lax.axis_size("dp")
    tensors = lax.axis_size("tensor")
    tensor_index = lax.axis_index("tensor")
    owner_index = lax.axis_index(OWNER_AXES)
    episodes = token_counts.shape[0]
    own_span = EP_LEN // tensors
    share = own_span * episodes
    capacity = max(2, 2 * episodes // owners)
    received = owners * capacity
    student_width = student_hidden.shape[1]
    width = student_width // owners
    tokens_all = EP_LEN * episodes * owners
    teacher_width = teacher_hidden.shape[1] * tensors

    id_rows = token_ids.reshape(own_span, episodes)
    looked = jnp.sum(
        jnp.where(
            id_rows[:, :, None] == jnp.arange(id_weight.shape[0], dtype=jnp.int32)[None, None, :],
            id_weight[None, None, :],
            0.0,
        ),
        axis=2,
    )
    position = tensor_index * own_span + jnp.arange(own_span, dtype=jnp.int32)[:, None]
    token_weight = jnp.where(position < token_counts[None, :], looked, 0.0).reshape(share, 1)

    own_rows = student_hidden.astype(jnp.float32)
    own_rescale = lax.rsqrt(jnp.mean(own_rows * own_rows, axis=1, keepdims=True) + EPSILON)
    owner_rows = jnp.tile(owner_map.astype(jnp.float32), (own_span, 1))
    extras = jnp.concatenate([token_weight, owner_rows, *three_terms(own_rescale)], axis=1)
    extras = jnp.pad(extras, ((0, 0), (0, EXTRA - extras.shape[1]))).astype(jnp.bfloat16)
    arrived = exchange(
        jnp.concatenate(
            [
                by_columns(student_hidden, owners),
                jnp.broadcast_to(extras[None], (owners, share, EXTRA)),
            ],
            axis=2,
        )
    )
    rows = owners * share
    student_block = arrived[:, :, :width].reshape(rows, width).astype(jnp.float32)
    facts = arrived[:, :, width:].astype(jnp.float32)
    weight_rows = facts[:, :, 0].reshape(rows, 1)
    owner_list = facts[:, :episodes, 1].astype(jnp.int32)
    rescale = (facts[:, :, 2] + facts[:, :, 3] + facts[:, :, 4]).reshape(rows, 1)
    gain = lax.dynamic_slice_in_dim(student_gain, owner_index * width, width, 0)
    normed = (student_block * rescale * gain[None, :]).astype(jnp.bfloat16)
    gathered = lax.all_gather(normed, "tensor", axis=0, tiled=True)

    widened = teacher_hidden.astype(jnp.float32)
    squares = jnp.sum(widened * widened, axis=1)
    scaled = (widened * teacher_gain[None, :]).astype(jnp.bfloat16)
    inverse = lax.rsqrt(lax.psum(squares, "tensor") / teacher_width + EPSILON)
    summed = lax.psum_scatter(
        jnp.dot(scaled, project_weight, preferred_element_type=jnp.float32).astype(jnp.bfloat16),
        "tensor",
        scatter_dimension=0,
        tiled=True,
    ).astype(jnp.float32)
    own_inverse = lax.dynamic_slice_in_dim(inverse, tensor_index * share, share, 0)
    projected = exchange(by_columns((summed * own_inverse[:, None]).astype(jnp.bfloat16), owners))

    hidden = gate_weight.shape[1]
    gate_part = jnp.dot(gathered, gate_weight, preferred_element_type=jnp.float32)
    up_part = jnp.dot(gathered, up_weight, preferred_element_type=jnp.float32)
    parts = jnp.stack(
        [
            gate_part.astype(jnp.bfloat16).reshape(owners, -1, hidden),
            up_part.astype(jnp.bfloat16).reshape(owners, -1, hidden),
        ],
        axis=1,
    )
    sums = lax.psum_scatter(parts, OWNER_AXES, scatter_dimension=0, tiled=True).astype(jnp.float32)
    activated = (jax.nn.silu(sums[0, 0]) * sums[0, 1]).astype(jnp.bfloat16)
    act_all = lax.all_gather(activated, OWNER_AXES, axis=0, tiled=True)
    branch = jnp.dot(act_all, down_weight, preferred_element_type=jnp.float32)
    branch_local = lax.psum_scatter(
        branch.astype(jnp.bfloat16), "tensor", scatter_dimension=0, tiled=True
    ).astype(jnp.float32)
    predicted = student_block + branch_local

    difference = predicted - projected.reshape(rows, width).astype(jnp.float32)
    grad_block = (weight_rows * difference * (1.0 / math.sqrt(tokens_all))).astype(jnp.bfloat16)
    grad_all = lax.all_gather(grad_block, "tensor", axis=0, tiled=True)
    down_grad = jnp.einsum("rc,rh->ch", grad_all, act_all, preferred_element_type=jnp.float32)

    selector = build_selector(owner_list, owners, capacity)
    picked = jnp.einsum(
        "sre,spef->sprf",
        selector,
        predicted.astype(jnp.bfloat16).reshape(owners, own_span, episodes, width),
        preferred_element_type=jnp.float32,
    ).astype(jnp.bfloat16)
    outgoing = picked.reshape(owners, own_span, owners, capacity, width).transpose(2, 1, 0, 3, 4)
    incoming = exchange(outgoing.reshape(owners, own_span, received, width))
    student_out = incoming.transpose(1, 2, 0, 3).reshape(1, own_span, received, student_width)
    return (student_out, down_grad)


MESH = pl.DeviceIdType.MESH
TILE = 256


def over_tiles(width, body):
    whole = width // TILE

    def step(index, carry):
        body(pl.multiple_of(index * TILE, TILE), TILE)
        return carry

    if whole:
        lax.fori_loop(0, whole, step, 0)
    if width > whole * TILE:
        body(whole * TILE, width - whole * TILE)


def column_of(row, eye):
    return jnp.sum(jnp.where(eye, row, 0.0), axis=1, keepdims=True)


def fused_kernel(
    size,
    teacher_ref,
    teacher_gain_ref,
    project_ref,
    student_ref,
    student_gain_ref,
    gate_ref,
    up_ref,
    down_ref,
    owner_ref,
    ids_ref,
    counts_ref,
    id_weight_ref,
    grad_out,
    act_out,
    student_out,
    th,
    scaled,
    pw,
    tp,
    st,
    nrm,
    gw,
    uw,
    dw,
    nb,
    own_part,
    d2s,
    d2r,
    own_x,
    xs,
    xr,
    act,
    bp,
    rss,
    rsr,
    trs,
    trr,
    sqs,
    sqr,
    inverse_ref,
    pjs,
    pj,
    sb,
    ext,
    ga,
    predb,
    sos,
    so,
    load_sem,
    nx_s,
    nx_r,
    raw_s,
    raw_r,
    ext_s,
    ext_r,
    pj_s,
    pj_r,
    so_s,
    so_r,
    sq_s,
    sq_r,
    ag_s,
    ag_r,
    tr_s,
    tr_r,
    rs_s,
    rs_r,
    gg_s,
    gg_r,
    d2_s,
    d2_r,
    x_s,
    x_r,
    a1_s,
    a1_r,
    a2_s,
    a2_r,
    a3_s,
    a3_r,
    out_sem,
):
    T, O, E, span, cap = size["T"], size["O"], size["E"], size["span"], size["cap"]
    share = span * E
    rows = O * share
    half, quarter = rows // 2, rows // 4
    W = nb.shape[2]
    H = gw.shape[0]
    DS = st.shape[1]
    t_half = share // 2
    f32, bf16 = jnp.float32, jnp.bfloat16

    x = lax.axis_index("group")
    c = lax.axis_index("dp")
    t = lax.axis_index("tensor")
    o = x * 2 + c
    odd = lax.rem(t, 2)
    r = (1 - odd) * lax.div(t, 2) + odd * (T - 1 - lax.div(t, 2))

    def at_ring(position):
        p = lax.rem(position, T)
        upper = lax.div(p, T // 2)
        return (1 - upper) * (2 * p) + upper * (2 * (T - 1 - p) + 1)

    nxt, prv = at_ring(r + 1), at_ring(r + T - 1)
    peers = (
        (1 - x, c, {"group": 1 - x}),
        (1 - x, 1 - c, {"group": 1 - x, "dp": 1 - c}),
        (x, 1 - c, {"dp": 1 - c}),
    )
    other_chip, core_peer = {"group": 1 - x}, {"dp": 1 - c}

    def remote(src, dst, send, recv, device):
        return pltpu.make_async_remote_copy(
            src_ref=src, dst_ref=dst, send_sem=send, recv_sem=recv, device_id=device, device_id_type=MESH
        )

    loads = [
        pltpu.make_async_copy(src, dst, load_sem.at[index])
        for index, (src, dst) in enumerate(
            [(student_ref, st), (teacher_ref, th), (project_ref, pw), (gate_ref, gw), (up_ref, uw), (down_ref, dw)]
        )
    ]
    for load in loads:
        load.start()

    barrier = pltpu.get_barrier_semaphore()
    for _, _, device in peers:
        pl.semaphore_signal(barrier, inc=1, device_id=device, device_id_type=MESH)
    for step in range(1, T):
        pl.semaphore_signal(barrier, inc=1, device_id={"tensor": at_ring(r + step)}, device_id_type=MESH)

    def columns(owner):
        return pl.ds(pl.multiple_of(owner * W, W), W)

    def owner_rows(owner):
        return pl.ds(pl.multiple_of(owner * share, share), share)

    def nx(k):
        return remote(
            nrm.at[:, columns(peers[k][0] * 2 + peers[k][1])],
            nb.at[0, owner_rows(o), :],
            nx_s.at[k],
            nx_r.at[k],
            peers[k][2],
        )

    def raw(k):
        return remote(
            st.at[:, columns(peers[k][0] * 2 + peers[k][1])],
            sb.at[owner_rows(o), :],
            raw_s.at[k],
            raw_r.at[k],
            peers[k][2],
        )

    def extra(k):
        return remote(ext.at[o], ext.at[o], ext_s.at[k], ext_r.at[k], peers[k][2])

    def proj(k):
        return remote(
            pjs.at[:, columns(peers[k][0] * 2 + peers[k][1])],
            pj.at[owner_rows(o), :],
            pj_s.at[k],
            pj_r.at[k],
            peers[k][2],
        )

    out_rows = span * O * cap

    def outgoing(k):
        q = peers[k][0] * 2 + peers[k][1]
        return remote(
            sos.at[pl.ds(pl.multiple_of(q * out_rows, out_rows), out_rows), :],
            so.at[:, columns(o)],
            so_s.at[k],
            so_r.at[k],
            peers[k][2],
        )

    def block_rows(position):
        return pl.ds(pl.multiple_of(at_ring(position) * share, share), share)

    def squares(step):
        return remote(
            sqs.at[block_rows(r + step), :],
            sqr.at[step],
            sq_s.at[step],
            sq_r.at[step],
            {"tensor": at_ring(r + step)},
        )

    def to(d):
        return {"tensor": nxt if d == 0 else prv}

    def part(d, n):
        return pl.ds(d * n, n)

    def ag(d, g):
        return remote(
            nb.at[g - 1, part(d, half), :], nb.at[g, part(d, half), :], ag_s.at[d, g], ag_r.at[d, g], to(d)
        )

    def rs(s, g):
        return remote(
            rss.at[g, part(s, share), :], rsr.at[g, part(s, share), :], rs_s.at[s, g], rs_r.at[s, g], to(s * 2 // O)
        )

    def tr(d, k):
        return remote(
            trs.at[k, part(d, t_half), :], trr.at[k, part(d, t_half), :], tr_s.at[d, k], tr_r.at[d, k], to(d)
        )

    def slot_of(d, s, k):
        return k if (d == 0) == (s < O // 2) else lax.rem(T - k, T)

    def gg(d, s, k):
        return remote(
            ga.at[slot_of(d, s, k - 1), part(s, share), :],
            ga.at[slot_of(d, s, k), part(s, share), :],
            gg_s.at[d * O + s, k],
            gg_r.at[d * O + s, k],
            to(d),
        )

    def gg_order():
        ahead, behind = list(range(O // 2)), list(range(O // 2, O))
        return [pair for a, b in zip(ahead + behind, behind + ahead) for pair in ((0, a), (1, b))]

    def goes_on(d, s):
        return (d == 0) == (s < O // 2)

    order = [s for pair in zip(range(O // 2), range(O // 2, O)) for s in pair]

    def d2(g, m):
        return remote(d2s.at[g, m], d2r.at[g, m], d2_s.at[m, g], d2_r.at[m, g], core_peer)

    def xch(g, m):
        return remote(xs.at[g, m], xr.at[g, m], x_s.at[m, g], x_r.at[m, g], other_chip)

    def act_rows(core, chip):
        return pl.ds(pl.multiple_of((core * 2 + chip) * quarter, quarter), quarter)

    own_act = act_rows(c, x)
    far_act = act_rows(c, 1 - x)

    def a1(g):
        return remote(act.at[g, own_act, :], act.at[g, own_act, :], a1_s.at[g], a1_r.at[g], other_chip)

    def a2(g):
        return remote(act.at[g, own_act, :], act.at[g, own_act, :], a2_s.at[g], a2_r.at[g], core_peer)

    def a3(g):
        return remote(act.at[g, far_act, :], act.at[g, far_act, :], a3_s.at[g], a3_r.at[g], core_peer)

    loads[0].wait()
    wide = st[...].astype(f32)
    rescale = lax.rsqrt(jnp.mean(wide * wide, axis=1, keepdims=True) + EPSILON)
    for j in range(DS // 128):
        lanes = slice(j * 128, (j + 1) * 128)
        nrm[:, lanes] = (wide[:, lanes] * rescale * student_gain_ref[j : j + 1, :]).astype(bf16)
    pl.semaphore_wait(barrier, len(peers) + T - 1)
    for k in range(len(peers)):
        nx(k).start()
    nb[0, owner_rows(o), :] = nrm[:, columns(o)]
    sb[owner_rows(o), :] = st[:, columns(o)]

    def iota(shape, axis):
        return lax.broadcasted_iota(jnp.int32, shape, axis)

    ids = ids_ref[...].astype(f32)
    ids_column = column_of(ids, iota((share, share), 0) == iota((share, share), 1))
    vocabulary = id_weight_ref.shape[1]
    looked = jnp.sum(
        jnp.where(ids_column == iota((share, vocabulary), 1).astype(f32), id_weight_ref[...], 0.0),
        axis=1,
        keepdims=True,
    )
    row_of = iota((share, E), 0)
    counts = column_of(counts_ref[...].astype(f32), lax.rem(row_of, E) == iota((share, E), 1))
    place = (t * span + lax.div(iota((share, 1), 0), E)).astype(f32)
    token_weight = jnp.where(place < counts, looked, 0.0).astype(bf16).astype(f32)
    own_column = column_of(owner_ref[...].astype(f32), iota((E, E), 0) == iota((E, E), 1))
    episode_row, episode_lane = iota((E, 128), 0), lax.rem(iota((E, 128), 1), E)
    own_lane = jnp.sum(jnp.where(episode_row == episode_lane, own_column, 0.0), axis=0, keepdims=True)
    rank = jnp.sum(
        jnp.where((own_column == own_lane) & (episode_row < episode_lane), 1.0, 0.0), axis=0, keepdims=True
    )
    target = own_lane * cap + rank
    ext[o, 0:share, :] = jnp.broadcast_to(token_weight, (share, 128))
    ext[o, share : share + 8, :] = jnp.broadcast_to(target, (8, 128))
    for k in range(len(peers)):
        raw(k).start()
        extra(k).start()

    loads[1].wait()
    wide = th[...].astype(f32)
    scaled[...] = (wide * teacher_gain_ref[...]).astype(bf16)
    sqs[...] = jnp.broadcast_to(jnp.sum(wide * wide, axis=1, keepdims=True), sqs.shape)
    for step in range(1, T):
        squares(step).start()
    loads[2].wait()

    def teacher_tile(offset, n):
        tp[:, pl.ds(offset, n)] = jnp.dot(
            scaled[...], pw[:, pl.ds(offset, n)], preferred_element_type=f32
        ).astype(bf16)

    def forward(k):
        @pl.when(k > 0)
        def _():
            ag(0, k).wait_recv()
            ag(1, k).wait_recv()

        @pl.when(k < T - 1)
        def _():
            ag(0, k + 1).start()
            ag(1, k + 1).start()

    whole = DS // TILE
    early = whole * 2 // 3

    def teacher_loop(index, carry):
        teacher_tile(pl.multiple_of(index * TILE, TILE), TILE)
        return carry

    lax.fori_loop(0, early, teacher_loop, 0)
    for k in range(len(peers)):
        nx(k).wait_recv()
    forward(0)

    def teacher_rest():
        lax.fori_loop(early, whole, teacher_loop, 0)
        if DS > whole * TILE:
            teacher_tile(whole * TILE, DS - whole * TILE)

    trr[0] = jnp.zeros(trr.shape[1:], bf16)
    rsr[0] = jnp.zeros(rsr.shape[1:], bf16)

    def teacher_rows(position, d):
        return pl.ds(pl.multiple_of(at_ring(position) * share + d * t_half, t_half), t_half)

    def teacher_step(k):
        @pl.when(k > 1)
        def _():
            tr(0, k - 1).wait_recv()
            tr(1, k - 1).wait_recv()

        for d in (0, 1):
            position = r + T - k if d == 0 else r + k
            trs[k, part(d, t_half), :] = (
                tp[teacher_rows(position, d), :].astype(f32) + trr[k - 1, part(d, t_half), :].astype(f32)
            ).astype(bf16)
            tr(d, k).start()

    loads[3].wait()
    loads[4].wait()
    loads[5].wait()

    def p1(g):
        away = pl.ds(pl.multiple_of((1 - c) * half, half), half)
        here = pl.ds(pl.multiple_of(c * half, half), half)
        for m, weight in enumerate((gw, uw)):

            def tile(offset, n):
                lhs = jnp.concatenate([nb[g, away, :], nb[g, here, :]], axis=0)
                value = lax.dot_general(
                    lhs, weight[pl.ds(offset, n), :], (((1,), (1,)), ((), ())), preferred_element_type=f32
                )
                d2s[g, m, :, pl.ds(offset, n)] = value[:half].astype(bf16)
                own_part[m, :, pl.ds(offset, n)] = value[half:]

            over_tiles(H, tile)
            d2(g, m).start()

    def p2(g):
        far = pl.ds(pl.multiple_of((1 - x) * quarter, quarter), quarter)
        near = pl.ds(pl.multiple_of(x * quarter, quarter), quarter)
        for m in (0, 1):
            d2(g, m).wait_recv()
            xs[g, m] = (own_part[m, far, :] + d2r[g, m, far, :].astype(f32)).astype(bf16)
            xch(g, m).start()
        for m in (0, 1):
            own_x[g, m] = own_part[m, near, :] + d2r[g, m, near, :].astype(f32)

    def p3(g):
        xch(g, 0).wait_recv()
        xch(g, 1).wait_recv()
        gate = own_x[g, 0] + xr[g, 0].astype(f32)
        up = own_x[g, 1] + xr[g, 1].astype(f32)
        act[g, own_act, :] = (gate / (1.0 + jnp.exp(-gate)) * up).astype(bf16)
        a1(g).start()
        a2(g).start()

    def p4(g):
        a1(g).wait_recv()
        a3(g).start()

    def act_store(g):
        return pltpu.make_async_copy(act.at[g], act_out.at[g], out_sem.at[0, g])

    def p5(g):
        a2(g).wait_recv()
        a3(g).wait_recv()
        act_store(g).start()

        kept = jnp.minimum(g, 1)

        def tile(offset, n):
            bp[kept, :, pl.ds(offset, n)] = jnp.dot(act[g], dw[:, pl.ds(offset, n)], preferred_element_type=f32)

        over_tiles(W, tile)

        @pl.when(g > 0)
        def _():
            for s in order:

                @pl.when(g > 1)
                def _():
                    rs(s, g - 1).wait_recv()

                own = part(s, share)
                rss[g, own, :] = (bp[1, own, :] + rsr[g - 1, own, :].astype(f32)).astype(bf16)
                rs(s, g).start()

    def finish_teacher():
        tr(0, T - 1).wait_recv()
        tr(1, T - 1).wait_recv()
        total = sqs[block_rows(r), :]
        for step in range(1, T):
            squares(step).wait_recv()
            total = total + sqr[step]
        inverse_ref[...] = lax.rsqrt(total * (1.0 / size["teacher_width"]) + EPSILON)
        for d in (0, 1):
            summed = tp[teacher_rows(r, d), :].astype(f32) + trr[T - 1, part(d, t_half), :].astype(f32)
            pjs[part(d, t_half), :] = (summed * inverse_ref[part(d, t_half), 0:1]).astype(bf16)
        for k in range(len(peers)):
            proj(k).start()
        pj[owner_rows(o), :] = pjs[:, columns(o)]

    first = T // 2

    def step(i, carry):
        @pl.when(i < T)
        def _():
            p1(i)

        @pl.when(i + 1 < T)
        def _():
            forward(i + 1)

        @pl.when((i >= 3) & (i < T + 3))
        def _():
            p4(i - 3)

        @pl.when(i == 0)
        def _():
            teacher_rest()

        @pl.when(i < first)
        def _():
            teacher_step(i + 1)

        @pl.when((i >= T - 1) & (i < T + T - 2 - first))
        def _():
            teacher_step(i - (T - 2 - first))

        @pl.when(i == T + T - 2 - first)
        def _():
            finish_teacher()

        @pl.when((i >= 2) & (i < T + 2))
        def _():
            p3(i - 2)

        @pl.when(i < T)
        def _():
            p2(i)

        @pl.when(i >= 3)
        def _():
            p5(i - 3)

        return carry

    lax.fori_loop(0, T + 3, step, 0)

    for k in range(len(peers)):
        raw(k).wait_recv()
        extra(k).wait_recv()
        proj(k).wait_recv()
    for s in order:
        rs(s, T - 1).wait_recv()
        own = slice(s * share, (s + 1) * share)
        predicted = sb[own, :].astype(f32) + (bp[0, own, :] + rsr[T - 1, own, :].astype(f32))
        predb[own, :] = predicted.astype(bf16)
        difference = predicted - pj[own, :].astype(f32)
        ga[0, own, :] = (ext[s, 0:share, 0:1] * difference * size["scale"]).astype(bf16)
        for d in (0, 1):
            gg(d, s, 1).start()

    def grad_store(g):
        return pltpu.make_async_copy(ga.at[g], grad_out.at[g], out_sem.at[1, g])

    grad_store(0).start()

    lane = iota((1, rows), 1)
    wanted_target = jnp.zeros((1, rows), f32)
    for s in range(O):
        wanted_target = jnp.where(lax.div(lane, share) == s, ext[s, share : share + 1, :], wanted_target)
    picks = O * out_rows
    line = iota((picks, rows), 0)
    place_row = lax.rem(lax.div(line, O * cap), span)
    source_row = lax.rem(lax.div(line, cap), O)
    slot = (lax.div(line, out_rows) * cap + lax.rem(line, cap)).astype(f32)
    lanes = iota((picks, rows), 1)
    chosen = (
        (wanted_target == slot)
        & (lax.div(lanes, share) == source_row)
        & (lax.div(lax.rem(lanes, share), E) == place_row)
    )
    selector = jnp.where(chosen, 1.0, 0.0).astype(bf16)

    def pick_tile(offset, n):
        sos[:, pl.ds(offset, n)] = jnp.dot(
            selector, predb[:, pl.ds(offset, n)], preferred_element_type=f32
        ).astype(bf16)

    over_tiles(W, pick_tile)
    for k in range(len(peers)):
        outgoing(k).start()
    so[:, columns(o)] = sos[pl.ds(pl.multiple_of(o * out_rows, out_rows), out_rows), :]

    far_hop = T // 2

    def gather_step(k, carry):
        for d, s in gg_order():
            if goes_on(d, s):
                gg(d, s, k).wait_recv()

                @pl.when(k < far_hop)
                def _():
                    gg(d, s, k + 1).start()
            else:

                @pl.when(k < far_hop)
                def _():
                    gg(d, s, k).wait_recv()

                @pl.when(k < far_hop - 1)
                def _():
                    gg(d, s, k + 1).start()

        grad_store(k).start()

        @pl.when(k < far_hop)
        def _():
            grad_store(T - k).start()

        return carry

    lax.fori_loop(1, far_hop + 1, gather_step, 0)

    for k in range(len(peers)):
        outgoing(k).wait_recv()
    student_store = pltpu.make_async_copy(so, student_out, out_sem.at[0, T])
    student_store.start()

    def drain(g, carry):
        for copy in (a1, a2, a3):
            copy(g).wait_send()
        for m in (0, 1):
            d2(g, m).wait_send()
            xch(g, m).wait_send()
        act_store(g).wait()
        grad_store(g).wait()

        @pl.when(g > 0)
        def _():
            squares(g).wait_send()
            for d in (0, 1):
                ag(d, g).wait_send()
                tr(d, g).wait_send()
            for s in range(O):
                rs(s, g).wait_send()

        @pl.when((g > 0) & (g <= far_hop))
        def _():
            for d, s in gg_order():
                if goes_on(d, s):
                    gg(d, s, g).wait_send()
                else:

                    @pl.when(g < far_hop)
                    def _():
                        gg(d, s, g).wait_send()

        return carry

    lax.fori_loop(0, T, drain, 0)
    for k in range(len(peers)):
        nx(k).wait_send()
        raw(k).wait_send()
        extra(k).wait_send()
        proj(k).wait_send()
        outgoing(k).wait_send()
    student_store.wait()


def fused(
    teacher_hidden,
    teacher_gain,
    project_weight,
    student_hidden,
    student_gain,
    gate_weight,
    up_weight,
    down_weight,
    owner_map,
    token_ids,
    token_counts,
    id_weight,
):
    f32, bf16 = jnp.float32, jnp.bfloat16
    T, O = lax.axis_size("tensor"), lax.axis_size("group") * lax.axis_size("dp")
    E = token_counts.shape[0]
    span = EP_LEN // T
    share = span * E
    rows = O * share
    half, quarter = rows // 2, rows // 4
    cap = max(2, 2 * E // O)
    local_tokens, F = teacher_hidden.shape
    DS = student_hidden.shape[1]
    W, H = gate_weight.shape
    out_rows = span * O * cap
    size = dict(
        T=T,
        O=O,
        E=E,
        span=span,
        cap=cap,
        teacher_width=F * T,
        scale=1.0 / math.sqrt(EP_LEN * E * O),
    )
    vmem = pl.BlockSpec(memory_space=pltpu.VMEM)
    anywhere = pl.BlockSpec(memory_space=pl.ANY)
    DMA = pltpu.SemaphoreType.DMA
    scratch = [
        pltpu.VMEM((local_tokens, F), bf16),
        pltpu.VMEM((local_tokens, F), bf16),
        pltpu.VMEM((F, DS), bf16),
        pltpu.VMEM((local_tokens, DS), bf16),
        pltpu.VMEM((share, DS), bf16),
        pltpu.VMEM((share, DS), bf16),
        pltpu.VMEM((H, W), bf16),
        pltpu.VMEM((H, W), bf16),
        pltpu.VMEM((H, W), bf16),
        pltpu.VMEM((T, rows, W), bf16),
        pltpu.VMEM((2, half, H), f32),
        pltpu.VMEM((T, 2, half, H), bf16),
        pltpu.VMEM((T, 2, half, H), bf16),
        pltpu.VMEM((T, 2, quarter, H), f32),
        pltpu.VMEM((T, 2, quarter, H), bf16),
        pltpu.VMEM((T, 2, quarter, H), bf16),
        pltpu.VMEM((T, rows, H), bf16),
        pltpu.VMEM((2, rows, W), f32),
        pltpu.VMEM((T, rows, W), bf16),
        pltpu.VMEM((T, rows, W), bf16),
        pltpu.VMEM((T, share, DS), bf16),
        pltpu.VMEM((T, share, DS), bf16),
        pltpu.VMEM((local_tokens, 128), f32),
        pltpu.VMEM((T, share, 128), f32),
        pltpu.VMEM((share, 128), f32),
        pltpu.VMEM((share, DS), bf16),
        pltpu.VMEM((rows, W), bf16),
        pltpu.VMEM((rows, W), bf16),
        pltpu.VMEM((O, share + 8, 128), f32),
        pltpu.VMEM((T, rows, W), bf16),
        pltpu.VMEM((rows, W), bf16),
        pltpu.VMEM((O * out_rows, W), bf16),
        pltpu.VMEM((out_rows, DS), bf16),
        DMA((6,)),
        *[DMA((3,)) for _ in range(10)],
        *[DMA((T,)) for _ in range(2)],
        *[DMA((2, T)) for _ in range(4)],
        *[DMA((O, T)) for _ in range(2)],
        *[DMA((2 * O, T // 2 + 1)) for _ in range(2)],
        *[DMA((2, T)) for _ in range(4)],
        *[DMA((T,)) for _ in range(6)],
        DMA((2, T + 1)),
    ]
    grads, acts, out = pl.pallas_call(
        functools.partial(fused_kernel, size),
        out_shape=(
            jax.ShapeDtypeStruct((T, rows, W), bf16),
            jax.ShapeDtypeStruct((T, rows, H), bf16),
            jax.ShapeDtypeStruct((out_rows, DS), bf16),
        ),
        in_specs=[anywhere, vmem, anywhere, anywhere, vmem, anywhere, anywhere, anywhere, vmem, vmem, vmem, vmem],
        out_specs=(anywhere, anywhere, anywhere),
        scratch_shapes=scratch,
        compiler_params=pltpu.CompilerParams(
            collective_id=0, has_side_effects=True, vmem_limit_bytes=63 * 1024 * 1024
        ),
    )(
        teacher_hidden,
        teacher_gain.reshape(1, F),
        project_weight,
        student_hidden,
        student_gain.reshape(DS // 128, 128),
        gate_weight.T,
        up_weight.T,
        down_weight,
        owner_map.reshape(1, E),
        token_ids.reshape(1, share),
        token_counts.reshape(1, E),
        id_weight.reshape(1, -1),
    )
    down_grad = jnp.einsum(
        "rc,rh->ch", grads.reshape(T * rows, W), acts.reshape(T * rows, H), preferred_element_type=f32
    )
    return (out.reshape(1, span, O * cap, DS), down_grad)


def fits(mesh):
    return mesh.shape["group"] == 2 and mesh.shape["dp"] == 2 and mesh.shape["tensor"] == 8


def solution(mesh):
    in_specs = (
        P(("group", "dp"), "tensor"),
        P("tensor"),
        P("tensor", None),
        P(("group", "dp", "tensor"), None),
        P(),
        P(("group", "dp"), "tensor"),
        P(("group", "dp"), "tensor"),
        P("tensor", ("group", "dp")),
        P(("group", "dp"), None),
        P(("group", "dp", "tensor")),
        P(("group", "dp")),
        P(),
    )
    out_specs = (P(("group", "dp"), "tensor", None, None), P(("group", "dp"), "tensor"))
    body = fused if fits(mesh) else general
    return jax.shard_map(body, mesh=mesh, in_specs=in_specs, out_specs=out_specs, check_vma=False)
```

```python
import functools
import math

import jax
import jax.numpy as jnp
from jax import lax
from jax.experimental import pallas as pl
from jax.experimental.pallas import tpu as pltpu
from jax.sharding import PartitionSpec as P

EP_LEN = 16
EXTRA = 128
EPSILON = 1e-06
OWNER_AXES = ("group", "dp")


def exchange(blocks):
    return lax.all_to_all(blocks, OWNER_AXES, split_axis=0, concat_axis=0, tiled=True)


def by_columns(rows, owners):
    return rows.reshape(rows.shape[0], owners, -1).transpose(1, 0, 2)


def three_terms(values):
    high = lax.reduce_precision(values, 8, 7)
    rest = values - high
    middle = lax.reduce_precision(rest, 8, 7)
    return high, middle, rest - middle


def build_selector(owner_list, owners, capacity):
    onehot = (owner_list[:, :, None] == jnp.arange(owners, dtype=jnp.int32)).astype(jnp.int32)
    earlier = jnp.cumsum(onehot, axis=1) - onehot
    rank_list = jnp.sum(earlier * onehot, axis=2)
    target = owner_list * capacity + rank_list
    slots = jnp.arange(owners * capacity, dtype=jnp.int32)
    return (target[:, None, :] == slots[None, :, None]).astype(jnp.bfloat16)


def general(
    teacher_hidden,
    teacher_gain,
    project_weight,
    student_hidden,
    student_gain,
    gate_weight,
    up_weight,
    down_weight,
    owner_map,
    token_ids,
    token_counts,
    id_weight,
):
    owners = lax.axis_size("group") * lax.axis_size("dp")
    tensors = lax.axis_size("tensor")
    tensor_index = lax.axis_index("tensor")
    owner_index = lax.axis_index(OWNER_AXES)
    episodes = token_counts.shape[0]
    own_span = EP_LEN // tensors
    share = own_span * episodes
    capacity = max(2, 2 * episodes // owners)
    received = owners * capacity
    student_width = student_hidden.shape[1]
    width = student_width // owners
    tokens_all = EP_LEN * episodes * owners
    teacher_width = teacher_hidden.shape[1] * tensors

    id_rows = token_ids.reshape(own_span, episodes)
    looked = jnp.sum(
        jnp.where(
            id_rows[:, :, None] == jnp.arange(id_weight.shape[0], dtype=jnp.int32)[None, None, :],
            id_weight[None, None, :],
            0.0,
        ),
        axis=2,
    )
    position = tensor_index * own_span + jnp.arange(own_span, dtype=jnp.int32)[:, None]
    token_weight = jnp.where(position < token_counts[None, :], looked, 0.0).reshape(share, 1)

    own_rows = student_hidden.astype(jnp.float32)
    own_rescale = lax.rsqrt(jnp.mean(own_rows * own_rows, axis=1, keepdims=True) + EPSILON)
    owner_rows = jnp.tile(owner_map.astype(jnp.float32), (own_span, 1))
    extras = jnp.concatenate([token_weight, owner_rows, *three_terms(own_rescale)], axis=1)
    extras = jnp.pad(extras, ((0, 0), (0, EXTRA - extras.shape[1]))).astype(jnp.bfloat16)
    arrived = exchange(
        jnp.concatenate(
            [
                by_columns(student_hidden, owners),
                jnp.broadcast_to(extras[None], (owners, share, EXTRA)),
            ],
            axis=2,
        )
    )
    rows = owners * share
    student_block = arrived[:, :, :width].reshape(rows, width).astype(jnp.float32)
    facts = arrived[:, :, width:].astype(jnp.float32)
    weight_rows = facts[:, :, 0].reshape(rows, 1)
    owner_list = facts[:, :episodes, 1].astype(jnp.int32)
    rescale = (facts[:, :, 2] + facts[:, :, 3] + facts[:, :, 4]).reshape(rows, 1)
    gain = lax.dynamic_slice_in_dim(student_gain, owner_index * width, width, 0)
    normed = (student_block * rescale * gain[None, :]).astype(jnp.bfloat16)
    gathered = lax.all_gather(normed, "tensor", axis=0, tiled=True)

    widened = teacher_hidden.astype(jnp.float32)
    squares = jnp.sum(widened * widened, axis=1)
    scaled = (widened * teacher_gain[None, :]).astype(jnp.bfloat16)
    inverse = lax.rsqrt(lax.psum(squares, "tensor") / teacher_width + EPSILON)
    summed = lax.psum_scatter(
        jnp.dot(scaled, project_weight, preferred_element_type=jnp.float32).astype(jnp.bfloat16),
        "tensor",
        scatter_dimension=0,
        tiled=True,
    ).astype(jnp.float32)
    own_inverse = lax.dynamic_slice_in_dim(inverse, tensor_index * share, share, 0)
    projected = exchange(by_columns((summed * own_inverse[:, None]).astype(jnp.bfloat16), owners))

    hidden = gate_weight.shape[1]
    gate_part = jnp.dot(gathered, gate_weight, preferred_element_type=jnp.float32)
    up_part = jnp.dot(gathered, up_weight, preferred_element_type=jnp.float32)
    parts = jnp.stack(
        [
            gate_part.astype(jnp.bfloat16).reshape(owners, -1, hidden),
            up_part.astype(jnp.bfloat16).reshape(owners, -1, hidden),
        ],
        axis=1,
    )
    sums = lax.psum_scatter(parts, OWNER_AXES, scatter_dimension=0, tiled=True).astype(jnp.float32)
    activated = (jax.nn.silu(sums[0, 0]) * sums[0, 1]).astype(jnp.bfloat16)
    act_all = lax.all_gather(activated, OWNER_AXES, axis=0, tiled=True)
    branch = jnp.dot(act_all, down_weight, preferred_element_type=jnp.float32)
    branch_local = lax.psum_scatter(
        branch.astype(jnp.bfloat16), "tensor", scatter_dimension=0, tiled=True
    ).astype(jnp.float32)
    predicted = student_block + branch_local

    difference = predicted - projected.reshape(rows, width).astype(jnp.float32)
    grad_block = (weight_rows * difference * (1.0 / math.sqrt(tokens_all))).astype(jnp.bfloat16)
    grad_all = lax.all_gather(grad_block, "tensor", axis=0, tiled=True)
    down_grad = jnp.einsum("rc,rh->ch", grad_all, act_all, preferred_element_type=jnp.float32)

    selector = build_selector(owner_list, owners, capacity)
    picked = jnp.einsum(
        "sre,spef->sprf",
        selector,
        predicted.astype(jnp.bfloat16).reshape(owners, own_span, episodes, width),
        preferred_element_type=jnp.float32,
    ).astype(jnp.bfloat16)
    outgoing = picked.reshape(owners, own_span, owners, capacity, width).transpose(2, 1, 0, 3, 4)
    incoming = exchange(outgoing.reshape(owners, own_span, received, width))
    student_out = incoming.transpose(1, 2, 0, 3).reshape(1, own_span, received, student_width)
    return (student_out, down_grad)


MESH = pl.DeviceIdType.MESH
TILE = 1024
TAIL = 256


def over_tiles(width, body):
    whole = width // TILE

    def step(index, carry):
        body(pl.multiple_of(index * TILE, TILE), TILE)
        return carry

    if whole:
        lax.fori_loop(0, whole, step, 0)
    if width > whole * TILE:
        body(whole * TILE, width - whole * TILE)


def column_of(row, eye):
    return jnp.sum(jnp.where(eye, row, 0.0), axis=1, keepdims=True)


def fused_kernel(
    size,
    teacher_ref,
    teacher_gain_ref,
    project_ref,
    student_ref,
    student_gain_ref,
    gate_ref,
    up_ref,
    down_ref,
    owner_ref,
    ids_ref,
    counts_ref,
    id_weight_ref,
    grad_out,
    act_out,
    student_out,
    sum_out,
    th,
    scaled,
    pw,
    tp,
    st,
    nrm,
    gw,
    uw,
    dw,
    nb,
    own_part,
    d2s,
    d2r,
    own_x,
    xs,
    xr,
    act,
    bp,
    rss,
    rsr,
    trs,
    trr,
    sqs,
    sqr,
    inverse_ref,
    pjs,
    pj,
    sb,
    ext,
    ga,
    act_t,
    acc,
    predb,
    sos,
    so,
    load_sem,
    nx_s,
    nx_r,
    raw_s,
    raw_r,
    ext_s,
    ext_r,
    pj_s,
    pj_r,
    so_s,
    so_r,
    sq_s,
    sq_r,
    ag_s,
    ag_r,
    tr_s,
    tr_r,
    rs_s,
    rs_r,
    gg_s,
    gg_r,
    d2_s,
    d2_r,
    x_s,
    x_r,
    a1_s,
    a1_r,
    a2_s,
    a2_r,
    a3_s,
    a3_r,
    out_sem,
):
    T, O, E, span, cap = size["T"], size["O"], size["E"], size["span"], size["cap"]
    share = span * E
    rows = O * share
    half, quarter = rows // 2, rows // 4
    W = nb.shape[2]
    H = gw.shape[0]
    DS = st.shape[1]
    t_half = share // 2
    f32, bf16 = jnp.float32, jnp.bfloat16

    x = lax.axis_index("group")
    c = lax.axis_index("dp")
    t = lax.axis_index("tensor")
    o = x * 2 + c
    odd = lax.rem(t, 2)
    r = (1 - odd) * lax.div(t, 2) + odd * (T - 1 - lax.div(t, 2))

    def at_ring(position):
        p = lax.rem(position, T)
        upper = lax.div(p, T // 2)
        return (1 - upper) * (2 * p) + upper * (2 * (T - 1 - p) + 1)

    nxt, prv = at_ring(r + 1), at_ring(r + T - 1)
    peers = (
        (1 - x, c, {"group": 1 - x}),
        (1 - x, 1 - c, {"group": 1 - x, "dp": 1 - c}),
        (x, 1 - c, {"dp": 1 - c}),
    )
    other_chip, core_peer = {"group": 1 - x}, {"dp": 1 - c}

    def remote(src, dst, send, recv, device):
        return pltpu.make_async_remote_copy(
            src_ref=src, dst_ref=dst, send_sem=send, recv_sem=recv, device_id=device, device_id_type=MESH
        )

    loads = [
        pltpu.make_async_copy(src, dst, load_sem.at[index])
        for index, (src, dst) in enumerate(
            [(student_ref, st), (teacher_ref, th), (project_ref, pw), (gate_ref, gw), (up_ref, uw), (down_ref, dw)]
        )
    ]
    for load in loads:
        load.start()

    barrier = pltpu.get_barrier_semaphore()
    for _, _, device in peers:
        pl.semaphore_signal(barrier, inc=1, device_id=device, device_id_type=MESH)
    for step in range(1, T):
        pl.semaphore_signal(barrier, inc=1, device_id={"tensor": at_ring(r + step)}, device_id_type=MESH)

    def columns(owner):
        return pl.ds(pl.multiple_of(owner * W, W), W)

    def owner_rows(owner):
        return pl.ds(pl.multiple_of(owner * share, share), share)

    def nx(k):
        return remote(
            nrm.at[:, columns(peers[k][0] * 2 + peers[k][1])],
            nb.at[0, owner_rows(o), :],
            nx_s.at[k],
            nx_r.at[k],
            peers[k][2],
        )

    def raw(k):
        return remote(
            st.at[:, columns(peers[k][0] * 2 + peers[k][1])],
            sb.at[owner_rows(o), :],
            raw_s.at[k],
            raw_r.at[k],
            peers[k][2],
        )

    def extra(k):
        return remote(ext.at[o], ext.at[o], ext_s.at[k], ext_r.at[k], peers[k][2])

    def proj(k):
        return remote(
            pjs.at[:, columns(peers[k][0] * 2 + peers[k][1])],
            pj.at[owner_rows(o), :],
            pj_s.at[k],
            pj_r.at[k],
            peers[k][2],
        )

    out_rows = span * O * cap

    def outgoing(k):
        q = peers[k][0] * 2 + peers[k][1]
        return remote(
            sos.at[pl.ds(pl.multiple_of(q * out_rows, out_rows), out_rows), :],
            so.at[:, columns(o)],
            so_s.at[k],
            so_r.at[k],
            peers[k][2],
        )

    def block_rows(position):
        return pl.ds(pl.multiple_of(at_ring(position) * share, share), share)

    def squares(step):
        return remote(
            sqs.at[block_rows(r + step), :],
            sqr.at[step],
            sq_s.at[step],
            sq_r.at[step],
            {"tensor": at_ring(r + step)},
        )

    def to(d):
        return {"tensor": nxt if d == 0 else prv}

    def part(d, n):
        return pl.ds(d * n, n)

    def ag(d, g):
        return remote(
            nb.at[g - 1, part(d, half), :], nb.at[g, part(d, half), :], ag_s.at[d, g], ag_r.at[d, g], to(d)
        )

    def rs(s, g):
        return remote(
            rss.at[g, part(s, share), :], rsr.at[g, part(s, share), :], rs_s.at[s, g], rs_r.at[s, g], to(s * 2 // O)
        )

    def tr(d, k):
        return remote(
            trs.at[k, part(d, t_half), :], trr.at[k, part(d, t_half), :], tr_s.at[d, k], tr_r.at[d, k], to(d)
        )

    def slot_of(d, s, k):
        return k if (d == 0) == (s < O // 2) else lax.rem(T - k, T)

    def gg(d, s, k):
        return remote(
            ga.at[slot_of(d, s, k - 1), part(s, share), :],
            ga.at[slot_of(d, s, k), part(s, share), :],
            gg_s.at[d * O + s, k],
            gg_r.at[d * O + s, k],
            to(d),
        )

    def gg_order():
        ahead, behind = list(range(O // 2)), list(range(O // 2, O))
        return [pair for a, b in zip(ahead + behind, behind + ahead) for pair in ((0, a), (1, b))]

    def goes_on(d, s):
        return (d == 0) == (s < O // 2)

    order = [s for pair in zip(range(O // 2), range(O // 2, O)) for s in pair]

    def d2(g, m):
        return remote(d2s.at[g, m], d2r.at[g, m], d2_s.at[m, g], d2_r.at[m, g], core_peer)

    def xch(g, m):
        return remote(xs.at[g, m], xr.at[g, m], x_s.at[m, g], x_r.at[m, g], other_chip)

    def act_rows(core, chip):
        return pl.ds(pl.multiple_of((core * 2 + chip) * quarter, quarter), quarter)

    own_act = act_rows(c, x)
    far_act = act_rows(c, 1 - x)

    def a1(g):
        return remote(act.at[g, own_act, :], act.at[g, own_act, :], a1_s.at[g], a1_r.at[g], other_chip)

    def a2(g):
        return remote(act.at[g, own_act, :], act.at[g, own_act, :], a2_s.at[g], a2_r.at[g], core_peer)

    def a3(g):
        return remote(act.at[g, far_act, :], act.at[g, far_act, :], a3_s.at[g], a3_r.at[g], core_peer)

    loads[0].wait()
    wide = st[...].astype(f32)
    rescale = lax.rsqrt(jnp.mean(wide * wide, axis=1, keepdims=True) + EPSILON)
    for j in range(DS // 128):
        lanes = slice(j * 128, (j + 1) * 128)
        nrm[:, lanes] = (wide[:, lanes] * rescale * student_gain_ref[j : j + 1, :]).astype(bf16)
    pl.semaphore_wait(barrier, len(peers) + T - 1)
    for k in range(len(peers)):
        nx(k).start()
    nb[0, owner_rows(o), :] = nrm[:, columns(o)]
    sb[owner_rows(o), :] = st[:, columns(o)]

    def iota(shape, axis):
        return lax.broadcasted_iota(jnp.int32, shape, axis)

    ids = ids_ref[...].astype(f32)
    ids_column = column_of(ids, iota((share, share), 0) == iota((share, share), 1))
    vocabulary = id_weight_ref.shape[1]
    looked = jnp.sum(
        jnp.where(ids_column == iota((share, vocabulary), 1).astype(f32), id_weight_ref[...], 0.0),
        axis=1,
        keepdims=True,
    )
    row_of = iota((share, E), 0)
    counts = column_of(counts_ref[...].astype(f32), lax.rem(row_of, E) == iota((share, E), 1))
    place = (t * span + lax.div(iota((share, 1), 0), E)).astype(f32)
    token_weight = jnp.where(place < counts, looked, 0.0).astype(bf16).astype(f32)
    own_column = column_of(owner_ref[...].astype(f32), iota((E, E), 0) == iota((E, E), 1))
    episode_row, episode_lane = iota((E, 128), 0), lax.rem(iota((E, 128), 1), E)
    own_lane = jnp.sum(jnp.where(episode_row == episode_lane, own_column, 0.0), axis=0, keepdims=True)
    rank = jnp.sum(
        jnp.where((own_column == own_lane) & (episode_row < episode_lane), 1.0, 0.0), axis=0, keepdims=True
    )
    target = own_lane * cap + rank
    ext[o, 0:share, :] = jnp.broadcast_to(token_weight, (share, 128))
    ext[o, share : share + 8, :] = jnp.broadcast_to(target, (8, 128))
    for k in range(len(peers)):
        raw(k).start()
        extra(k).start()

    loads[1].wait()
    wide = th[...].astype(f32)
    scaled[...] = (wide * teacher_gain_ref[...]).astype(bf16)
    sqs[...] = jnp.broadcast_to(jnp.sum(wide * wide, axis=1, keepdims=True), sqs.shape)
    for step in range(1, T):
        squares(step).start()
    loads[2].wait()

    def teacher_tile(offset, n):
        tp[:, pl.ds(offset, n)] = jnp.dot(
            scaled[...], pw[:, pl.ds(offset, n)], preferred_element_type=f32
        ).astype(bf16)

    def forward(k):
        @pl.when(k > 0)
        def _():
            ag(0, k).wait_recv()
            ag(1, k).wait_recv()

        @pl.when(k < T - 1)
        def _():
            ag(0, k + 1).start()
            ag(1, k + 1).start()

    whole = DS // TILE
    early = whole * 2 // 3

    def teacher_loop(index, carry):
        teacher_tile(pl.multiple_of(index * TILE, TILE), TILE)
        return carry

    lax.fori_loop(0, early, teacher_loop, 0)
    for k in range(len(peers)):
        nx(k).wait_recv()
    forward(0)

    def teacher_rest():
        lax.fori_loop(early, whole, teacher_loop, 0)
        if DS > whole * TILE:
            teacher_tile(whole * TILE, DS - whole * TILE)

    trr[0] = jnp.zeros(trr.shape[1:], bf16)
    rsr[0] = jnp.zeros(rsr.shape[1:], bf16)

    def teacher_rows(position, d):
        return pl.ds(pl.multiple_of(at_ring(position) * share + d * t_half, t_half), t_half)

    def teacher_step(k):
        @pl.when(k > 1)
        def _():
            tr(0, k - 1).wait_recv()
            tr(1, k - 1).wait_recv()

        for d in (0, 1):
            position = r + T - k if d == 0 else r + k
            trs[k, part(d, t_half), :] = (
                tp[teacher_rows(position, d), :].astype(f32) + trr[k - 1, part(d, t_half), :].astype(f32)
            ).astype(bf16)
            tr(d, k).start()

    loads[3].wait()
    loads[4].wait()
    loads[5].wait()

    def p1(g):
        away = pl.ds(pl.multiple_of((1 - c) * half, half), half)
        here = pl.ds(pl.multiple_of(c * half, half), half)
        for m, weight in enumerate((gw, uw)):

            def tile(offset, n):
                lhs = jnp.concatenate([nb[g, away, :], nb[g, here, :]], axis=0)
                value = lax.dot_general(
                    lhs, weight[pl.ds(offset, n), :], (((1,), (1,)), ((), ())), preferred_element_type=f32
                )
                d2s[g, m, :, pl.ds(offset, n)] = value[:half].astype(bf16)
                own_part[m, :, pl.ds(offset, n)] = value[half:]

            over_tiles(H, tile)
            d2(g, m).start()

    def p2(g):
        far = pl.ds(pl.multiple_of((1 - x) * quarter, quarter), quarter)
        near = pl.ds(pl.multiple_of(x * quarter, quarter), quarter)
        for m in (0, 1):
            d2(g, m).wait_recv()
            xs[g, m] = (own_part[m, far, :] + d2r[g, m, far, :].astype(f32)).astype(bf16)
            xch(g, m).start()
        for m in (0, 1):
            own_x[g, m] = own_part[m, near, :] + d2r[g, m, near, :].astype(f32)

    def p3(g):
        xch(g, 0).wait_recv()
        xch(g, 1).wait_recv()
        gate = own_x[g, 0] + xr[g, 0].astype(f32)
        up = own_x[g, 1] + xr[g, 1].astype(f32)
        act[g, own_act, :] = (gate / (1.0 + jnp.exp(-gate)) * up).astype(bf16)
        a1(g).start()
        a2(g).start()

    def p4(g):
        a1(g).wait_recv()
        a3(g).start()

    far_hop = T // 2
    act_store = pltpu.make_async_copy(act_t.at[far_hop], act_out, out_sem.at[0])

    def p5(g):
        a2(g).wait_recv()
        a3(g).wait_recv()

        kept = jnp.minimum(g, 1)

        def tile(offset, n):
            bp[kept, :, pl.ds(offset, n)] = jnp.dot(act[g], dw[:, pl.ds(offset, n)], preferred_element_type=f32)

        over_tiles(W, tile)

        @pl.when(g > 0)
        def _():
            for s in order:

                @pl.when(g > 1)
                def _():
                    rs(s, g - 1).wait_recv()

                own = part(s, share)
                rss[g, own, :] = (bp[1, own, :] + rsr[g - 1, own, :].astype(f32)).astype(bf16)
                rs(s, g).start()

        act_t[g] = act[g].T

        @pl.when(g == far_hop)
        def _():
            act_store.start()

    def finish_teacher():
        tr(0, T - 1).wait_recv()
        tr(1, T - 1).wait_recv()
        total = sqs[block_rows(r), :]
        for step in range(1, T):
            squares(step).wait_recv()
            total = total + sqr[step]
        inverse_ref[...] = lax.rsqrt(total * (1.0 / size["teacher_width"]) + EPSILON)
        for d in (0, 1):
            summed = tp[teacher_rows(r, d), :].astype(f32) + trr[T - 1, part(d, t_half), :].astype(f32)
            pjs[part(d, t_half), :] = (summed * inverse_ref[part(d, t_half), 0:1]).astype(bf16)
        for k in range(len(peers)):
            proj(k).start()
        pj[owner_rows(o), :] = pjs[:, columns(o)]

    first = T // 2

    def step(i, carry):
        @pl.when(i < T)
        def _():
            p1(i)

        @pl.when(i + 1 < T)
        def _():
            forward(i + 1)

        @pl.when((i >= 3) & (i < T + 3))
        def _():
            p4(i - 3)

        @pl.when((i >= T - 1) & (i < T + T - 2 - first))
        def _():
            teacher_step(i - (T - 2 - first))

        @pl.when(i == T + T - 2 - first)
        def _():
            finish_teacher()

        @pl.when((i >= 2) & (i < T + 2))
        def _():
            p3(i - 2)

        @pl.when(i < T)
        def _():
            p2(i)

        @pl.when(i < first)
        def _():
            @pl.when(i == 0)
            def _():
                teacher_rest()

            teacher_step(i + 1)

        @pl.when(i >= 3)
        def _():
            p5(i - 3)

        return carry

    lax.fori_loop(0, T + 3, step, 0)

    for k in range(len(peers)):
        raw(k).wait_recv()
        extra(k).wait_recv()
        proj(k).wait_recv()
    for s in order:
        rs(s, T - 1).wait_recv()
        own = slice(s * share, (s + 1) * share)
        predicted = sb[own, :].astype(f32) + (bp[0, own, :] + rsr[T - 1, own, :].astype(f32))
        predb[own, :] = predicted.astype(bf16)
        difference = predicted - pj[own, :].astype(f32)
        ga[0, own, :] = (ext[s, 0:share, 0:1] * difference * size["scale"]).astype(bf16)
        for d in (0, 1):
            gg(d, s, 1).start()

    grad_store = pltpu.make_async_copy(ga.at[far_hop], grad_out, out_sem.at[1])
    pieces = [slice(j, min(j + TAIL, W)) for j in range(0, W, TAIL)]
    sum_stores = [
        pltpu.make_async_copy(acc.at[:, lanes], sum_out.at[:, lanes], out_sem.at[3 + j])
        for j, lanes in enumerate(pieces)
    ]

    lane = iota((1, rows), 1)
    wanted_target = jnp.zeros((1, rows), f32)
    for s in range(O):
        wanted_target = jnp.where(lax.div(lane, share) == s, ext[s, share : share + 1, :], wanted_target)
    picks = O * out_rows
    line = iota((picks, rows), 0)
    place_row = lax.rem(lax.div(line, O * cap), span)
    source_row = lax.rem(lax.div(line, cap), O)
    slot = (lax.div(line, out_rows) * cap + lax.rem(line, cap)).astype(f32)
    lanes = iota((picks, rows), 1)
    chosen = (
        (wanted_target == slot)
        & (lax.div(lanes, share) == source_row)
        & (lax.div(lax.rem(lanes, share), E) == place_row)
    )
    selector = jnp.where(chosen, 1.0, 0.0).astype(bf16)

    def pick_tile(offset, n):
        sos[:, pl.ds(offset, n)] = jnp.dot(
            selector, predb[:, pl.ds(offset, n)], preferred_element_type=f32
        ).astype(bf16)

    over_tiles(W, pick_tile)
    for k in range(len(peers)):
        outgoing(k).start()
    so[:, columns(o)] = sos[pl.ds(pl.multiple_of(o * out_rows, out_rows), out_rows), :]

    def product(k, lanes):
        @pl.when(k == 0)
        def _():
            acc[:, lanes] = jnp.dot(act_t[0], ga[0, :, lanes], preferred_element_type=f32)

        @pl.when(k > 0)
        def _():
            near, back = jnp.maximum(k, 1), T - jnp.maximum(k, 1)
            lhs = jnp.concatenate([act_t[near], act_t[back]], axis=1)
            rhs = jnp.concatenate([ga[near, :, lanes], ga[back, :, lanes]], axis=0)
            acc[:, lanes] += jnp.dot(lhs, rhs, preferred_element_type=f32)

    def gather_step(k, carry):
        steps = gg_order()
        for index, (d, s) in enumerate(steps):
            if goes_on(d, s):
                gg(d, s, k).wait_recv()

                @pl.when(k < far_hop)
                def _():
                    gg(d, s, k + 1).start()
            else:

                @pl.when(k < far_hop)
                def _():
                    gg(d, s, k).wait_recv()

                @pl.when(k < far_hop - 1)
                def _():
                    gg(d, s, k + 1).start()

            for j in range(index * len(pieces) // len(steps), (index + 1) * len(pieces) // len(steps)):
                product(k - 1, pieces[j])

                @pl.when(k == far_hop)
                def _():
                    sum_stores[j].start()

        return carry

    lax.fori_loop(1, far_hop + 1, gather_step, 0)
    grad_store.start()

    for k in range(len(peers)):
        outgoing(k).wait_recv()
    student_store = pltpu.make_async_copy(so, student_out, out_sem.at[2])
    student_store.start()

    def drain(g, carry):
        for copy in (a1, a2, a3):
            copy(g).wait_send()
        for m in (0, 1):
            d2(g, m).wait_send()
            xch(g, m).wait_send()

        @pl.when(g > 0)
        def _():
            squares(g).wait_send()
            for d in (0, 1):
                ag(d, g).wait_send()
                tr(d, g).wait_send()
            for s in range(O):
                rs(s, g).wait_send()

        @pl.when((g > 0) & (g <= far_hop))
        def _():
            for d, s in gg_order():
                if goes_on(d, s):
                    gg(d, s, g).wait_send()
                else:

                    @pl.when(g < far_hop)
                    def _():
                        gg(d, s, g).wait_send()

        return carry

    lax.fori_loop(0, T, drain, 0)
    for k in range(len(peers)):
        nx(k).wait_send()
        raw(k).wait_send()
        extra(k).wait_send()
        proj(k).wait_send()
        outgoing(k).wait_send()
    for copy in (act_store, grad_store, student_store, *sum_stores):
        copy.wait()


def last_terms(
    sum_ref, act_ref, grad_ref, student_ref, out_ref, student_out, total, act, grad, student, small_sem, in_sem, out_sem
):
    height = total.shape[0]
    blocks = [pl.ds(j, min(TAIL, height - j)) for j in range(0, height, TAIL)]
    small = [
        pltpu.make_async_copy(act_ref, act, small_sem.at[0]),
        pltpu.make_async_copy(grad_ref, grad, small_sem.at[1]),
    ]
    student_load = pltpu.make_async_copy(student_ref, student, small_sem.at[2])
    student_store = pltpu.make_async_copy(student, student_out, small_sem.at[3])
    loads = [pltpu.make_async_copy(sum_ref.at[b, :], total.at[b, :], in_sem.at[j]) for j, b in enumerate(blocks)]
    stores = [pltpu.make_async_copy(total.at[b, :], out_ref.at[b, :], out_sem.at[j]) for j, b in enumerate(blocks)]
    for copy in (*small, *loads, student_load):
        copy.start()
    for copy in small:
        copy.wait()
    for b, load, store in zip(blocks, loads, stores):
        term = jnp.dot(act[b, :], grad[...], preferred_element_type=jnp.float32)
        load.wait()
        total[b, :] += term
        store.start()
    student_load.wait()
    student_store.start()
    for copy in (*stores, student_store):
        copy.wait()


def fused(
    teacher_hidden,
    teacher_gain,
    project_weight,
    student_hidden,
    student_gain,
    gate_weight,
    up_weight,
    down_weight,
    owner_map,
    token_ids,
    token_counts,
    id_weight,
):
    f32, bf16 = jnp.float32, jnp.bfloat16
    T, O = lax.axis_size("tensor"), lax.axis_size("group") * lax.axis_size("dp")
    E = token_counts.shape[0]
    span = EP_LEN // T
    share = span * E
    rows = O * share
    half, quarter = rows // 2, rows // 4
    cap = max(2, 2 * E // O)
    local_tokens, F = teacher_hidden.shape
    DS = student_hidden.shape[1]
    W, H = gate_weight.shape
    out_rows = span * O * cap
    size = dict(
        T=T,
        O=O,
        E=E,
        span=span,
        cap=cap,
        teacher_width=F * T,
        scale=1.0 / math.sqrt(EP_LEN * E * O),
    )
    vmem = pl.BlockSpec(memory_space=pltpu.VMEM)
    anywhere = pl.BlockSpec(memory_space=pl.ANY)
    DMA = pltpu.SemaphoreType.DMA
    scratch = [
        pltpu.VMEM((local_tokens, F), bf16),
        pltpu.VMEM((local_tokens, F), bf16),
        pltpu.VMEM((F, DS), bf16),
        pltpu.VMEM((local_tokens, DS), bf16),
        pltpu.VMEM((share, DS), bf16),
        pltpu.VMEM((share, DS), bf16),
        pltpu.VMEM((H, W), bf16),
        pltpu.VMEM((H, W), bf16),
        pltpu.VMEM((H, W), bf16),
        pltpu.VMEM((T, rows, W), bf16),
        pltpu.VMEM((2, half, H), f32),
        pltpu.VMEM((T, 2, half, H), bf16),
        pltpu.VMEM((T, 2, half, H), bf16),
        pltpu.VMEM((T, 2, quarter, H), f32),
        pltpu.VMEM((T, 2, quarter, H), bf16),
        pltpu.VMEM((T, 2, quarter, H), bf16),
        pltpu.VMEM((T, rows, H), bf16),
        pltpu.VMEM((2, rows, W), f32),
        pltpu.VMEM((T, rows, W), bf16),
        pltpu.VMEM((T, rows, W), bf16),
        pltpu.VMEM((T, share, DS), bf16),
        pltpu.VMEM((T, share, DS), bf16),
        pltpu.VMEM((local_tokens, 128), f32),
        pltpu.VMEM((T, share, 128), f32),
        pltpu.VMEM((share, 128), f32),
        pltpu.VMEM((share, DS), bf16),
        pltpu.VMEM((rows, W), bf16),
        pltpu.VMEM((rows, W), bf16),
        pltpu.VMEM((O, share + 8, 128), f32),
        pltpu.VMEM((T, rows, W), bf16),
        pltpu.VMEM((T, H, rows), bf16),
        pltpu.VMEM((H, W), f32),
        pltpu.VMEM((rows, W), bf16),
        pltpu.VMEM((O * out_rows, W), bf16),
        pltpu.VMEM((out_rows, DS), bf16),
        DMA((6,)),
        *[DMA((3,)) for _ in range(10)],
        *[DMA((T,)) for _ in range(2)],
        *[DMA((2, T)) for _ in range(4)],
        *[DMA((O, T)) for _ in range(2)],
        *[DMA((2 * O, T // 2 + 1)) for _ in range(2)],
        *[DMA((2, T)) for _ in range(4)],
        *[DMA((T,)) for _ in range(6)],
        DMA((3 + pl.cdiv(W, TAIL),)),
    ]
    grads, acts, out, summed = pl.pallas_call(
        functools.partial(fused_kernel, size),
        out_shape=(
            jax.ShapeDtypeStruct((rows, W), bf16),
            jax.ShapeDtypeStruct((H, rows), bf16),
            jax.ShapeDtypeStruct((out_rows, DS), bf16),
            jax.ShapeDtypeStruct((H, W), f32),
        ),
        in_specs=[anywhere, vmem, anywhere, anywhere, vmem, anywhere, anywhere, anywhere, vmem, vmem, vmem, vmem],
        out_specs=(anywhere, anywhere, anywhere, anywhere),
        scratch_shapes=scratch,
        compiler_params=pltpu.CompilerParams(
            collective_id=0, has_side_effects=True, vmem_limit_bytes=63 * 1024 * 1024
        ),
    )(
        teacher_hidden,
        teacher_gain.reshape(1, F),
        project_weight,
        student_hidden,
        student_gain.reshape(DS // 128, 128),
        gate_weight.T,
        up_weight.T,
        down_weight,
        owner_map.reshape(1, E),
        token_ids.reshape(1, share),
        token_counts.reshape(1, E),
        id_weight.reshape(1, -1),
    )
    blocks = pl.cdiv(H, TAIL)
    down_grad, out = pl.pallas_call(
        last_terms,
        out_shape=(jax.ShapeDtypeStruct((H, W), f32), jax.ShapeDtypeStruct((out_rows, DS), bf16)),
        in_specs=[anywhere] * 4,
        out_specs=(anywhere, anywhere),
        scratch_shapes=[
            pltpu.VMEM((H, W), f32),
            pltpu.VMEM((H, rows), bf16),
            pltpu.VMEM((rows, W), bf16),
            pltpu.VMEM((out_rows, DS), bf16),
            DMA((4,)),
            DMA((blocks,)),
            DMA((blocks,)),
        ],
        compiler_params=pltpu.CompilerParams(vmem_limit_bytes=63 * 1024 * 1024),
    )(summed, acts, grads, out)
    return (out.reshape(1, span, O * cap, DS), down_grad.T)


def fits(mesh):
    return mesh.shape["group"] == 2 and mesh.shape["dp"] == 2 and mesh.shape["tensor"] == 8


def solution(mesh):
    in_specs = (
        P(("group", "dp"), "tensor"),
        P("tensor"),
        P("tensor", None),
        P(("group", "dp", "tensor"), None),
        P(),
        P(("group", "dp"), "tensor"),
        P(("group", "dp"), "tensor"),
        P("tensor", ("group", "dp")),
        P(("group", "dp"), None),
        P(("group", "dp", "tensor")),
        P(("group", "dp")),
        P(),
    )
    out_specs = (P(("group", "dp"), "tensor", None, None), P(("group", "dp"), "tensor"))
    body = fused if fits(mesh) else general
    return jax.shard_map(body, mesh=mesh, in_specs=in_specs, out_specs=out_specs, check_vma=False)
```

```python
import functools
import math

import jax
import jax.numpy as jnp
from jax import lax
from jax.experimental import pallas as pl
from jax.experimental.pallas import tpu as pltpu
from jax.sharding import PartitionSpec as P

EP_LEN = 16
EXTRA = 128
EPSILON = 1e-06
OWNER_AXES = ("group", "dp")


def exchange(blocks):
    return lax.all_to_all(blocks, OWNER_AXES, split_axis=0, concat_axis=0, tiled=True)


def by_columns(rows, owners):
    return rows.reshape(rows.shape[0], owners, -1).transpose(1, 0, 2)


def three_terms(values):
    high = lax.reduce_precision(values, 8, 7)
    rest = values - high
    middle = lax.reduce_precision(rest, 8, 7)
    return high, middle, rest - middle


def build_selector(owner_list, owners, capacity):
    onehot = (owner_list[:, :, None] == jnp.arange(owners, dtype=jnp.int32)).astype(jnp.int32)
    earlier = jnp.cumsum(onehot, axis=1) - onehot
    rank_list = jnp.sum(earlier * onehot, axis=2)
    target = owner_list * capacity + rank_list
    slots = jnp.arange(owners * capacity, dtype=jnp.int32)
    return (target[:, None, :] == slots[None, :, None]).astype(jnp.bfloat16)


def general(
    teacher_hidden,
    teacher_gain,
    project_weight,
    student_hidden,
    student_gain,
    gate_weight,
    up_weight,
    down_weight,
    owner_map,
    token_ids,
    token_counts,
    id_weight,
):
    owners = lax.axis_size("group") * lax.axis_size("dp")
    tensors = lax.axis_size("tensor")
    tensor_index = lax.axis_index("tensor")
    owner_index = lax.axis_index(OWNER_AXES)
    episodes = token_counts.shape[0]
    own_span = EP_LEN // tensors
    share = own_span * episodes
    capacity = max(2, 2 * episodes // owners)
    received = owners * capacity
    student_width = student_hidden.shape[1]
    width = student_width // owners
    tokens_all = EP_LEN * episodes * owners
    teacher_width = teacher_hidden.shape[1] * tensors

    id_rows = token_ids.reshape(own_span, episodes)
    looked = jnp.sum(
        jnp.where(
            id_rows[:, :, None] == jnp.arange(id_weight.shape[0], dtype=jnp.int32)[None, None, :],
            id_weight[None, None, :],
            0.0,
        ),
        axis=2,
    )
    position = tensor_index * own_span + jnp.arange(own_span, dtype=jnp.int32)[:, None]
    token_weight = jnp.where(position < token_counts[None, :], looked, 0.0).reshape(share, 1)

    own_rows = student_hidden.astype(jnp.float32)
    own_rescale = lax.rsqrt(jnp.mean(own_rows * own_rows, axis=1, keepdims=True) + EPSILON)
    owner_rows = jnp.tile(owner_map.astype(jnp.float32), (own_span, 1))
    extras = jnp.concatenate([token_weight, owner_rows, *three_terms(own_rescale)], axis=1)
    extras = jnp.pad(extras, ((0, 0), (0, EXTRA - extras.shape[1]))).astype(jnp.bfloat16)
    arrived = exchange(
        jnp.concatenate(
            [
                by_columns(student_hidden, owners),
                jnp.broadcast_to(extras[None], (owners, share, EXTRA)),
            ],
            axis=2,
        )
    )
    rows = owners * share
    student_block = arrived[:, :, :width].reshape(rows, width).astype(jnp.float32)
    facts = arrived[:, :, width:].astype(jnp.float32)
    weight_rows = facts[:, :, 0].reshape(rows, 1)
    owner_list = facts[:, :episodes, 1].astype(jnp.int32)
    rescale = (facts[:, :, 2] + facts[:, :, 3] + facts[:, :, 4]).reshape(rows, 1)
    gain = lax.dynamic_slice_in_dim(student_gain, owner_index * width, width, 0)
    normed = (student_block * rescale * gain[None, :]).astype(jnp.bfloat16)
    gathered = lax.all_gather(normed, "tensor", axis=0, tiled=True)

    widened = teacher_hidden.astype(jnp.float32)
    squares = jnp.sum(widened * widened, axis=1)
    scaled = (widened * teacher_gain[None, :]).astype(jnp.bfloat16)
    inverse = lax.rsqrt(lax.psum(squares, "tensor") / teacher_width + EPSILON)
    summed = lax.psum_scatter(
        jnp.dot(scaled, project_weight, preferred_element_type=jnp.float32).astype(jnp.bfloat16),
        "tensor",
        scatter_dimension=0,
        tiled=True,
    ).astype(jnp.float32)
    own_inverse = lax.dynamic_slice_in_dim(inverse, tensor_index * share, share, 0)
    projected = exchange(by_columns((summed * own_inverse[:, None]).astype(jnp.bfloat16), owners))

    hidden = gate_weight.shape[1]
    gate_part = jnp.dot(gathered, gate_weight, preferred_element_type=jnp.float32)
    up_part = jnp.dot(gathered, up_weight, preferred_element_type=jnp.float32)
    parts = jnp.stack(
        [
            gate_part.astype(jnp.bfloat16).reshape(owners, -1, hidden),
            up_part.astype(jnp.bfloat16).reshape(owners, -1, hidden),
        ],
        axis=1,
    )
    sums = lax.psum_scatter(parts, OWNER_AXES, scatter_dimension=0, tiled=True).astype(jnp.float32)
    activated = (jax.nn.silu(sums[0, 0]) * sums[0, 1]).astype(jnp.bfloat16)
    act_all = lax.all_gather(activated, OWNER_AXES, axis=0, tiled=True)
    branch = jnp.dot(act_all, down_weight, preferred_element_type=jnp.float32)
    branch_local = lax.psum_scatter(
        branch.astype(jnp.bfloat16), "tensor", scatter_dimension=0, tiled=True
    ).astype(jnp.float32)
    predicted = student_block + branch_local

    difference = predicted - projected.reshape(rows, width).astype(jnp.float32)
    grad_block = (weight_rows * difference * (1.0 / math.sqrt(tokens_all))).astype(jnp.bfloat16)
    grad_all = lax.all_gather(grad_block, "tensor", axis=0, tiled=True)
    down_grad = jnp.einsum("rc,rh->ch", grad_all, act_all, preferred_element_type=jnp.float32)

    selector = build_selector(owner_list, owners, capacity)
    picked = jnp.einsum(
        "sre,spef->sprf",
        selector,
        predicted.astype(jnp.bfloat16).reshape(owners, own_span, episodes, width),
        preferred_element_type=jnp.float32,
    ).astype(jnp.bfloat16)
    outgoing = picked.reshape(owners, own_span, owners, capacity, width).transpose(2, 1, 0, 3, 4)
    incoming = exchange(outgoing.reshape(owners, own_span, received, width))
    student_out = incoming.transpose(1, 2, 0, 3).reshape(1, own_span, received, student_width)
    return (student_out, down_grad)


MESH = pl.DeviceIdType.MESH
TILE = 1024
TAIL = 256


def over_tiles(width, body):
    whole = width // TILE

    def step(index, carry):
        body(pl.multiple_of(index * TILE, TILE), TILE)
        return carry

    if whole:
        lax.fori_loop(0, whole, step, 0)
    if width > whole * TILE:
        body(whole * TILE, width - whole * TILE)


def column_of(row, eye):
    return jnp.sum(jnp.where(eye, row, 0.0), axis=1, keepdims=True)


def fused_kernel(
    size,
    teacher_ref,
    teacher_gain_in,
    project_ref,
    student_ref,
    student_gain_in,
    gate_ref,
    up_ref,
    down_ref,
    owner_in,
    ids_in,
    counts_in,
    id_weight_in,
    grad_out,
    act_out,
    student_out,
    sum_out,
    th,
    scaled,
    pw,
    tp,
    st,
    nrm,
    gw,
    uw,
    dw,
    nb,
    own_part,
    d2s,
    d2r,
    own_x,
    xs,
    xr,
    act,
    bp,
    rss,
    rsr,
    trs,
    trr,
    sqs,
    sqr,
    inverse_ref,
    pjs,
    pj,
    sb,
    ext,
    ga,
    act_t,
    acc,
    predb,
    sos,
    so,
    student_gain_ref,
    owner_ref,
    ids_ref,
    counts_ref,
    id_weight_ref,
    teacher_gain_ref,
    load_sem,
    nx_s,
    nx_r,
    raw_s,
    raw_r,
    ext_s,
    ext_r,
    pj_s,
    pj_r,
    so_s,
    so_r,
    sq_s,
    sq_r,
    ag_s,
    ag_r,
    tr_s,
    tr_r,
    rs_s,
    rs_r,
    gg_s,
    gg_r,
    d2_s,
    d2_r,
    x_s,
    x_r,
    a1_s,
    a1_r,
    a2_s,
    a2_r,
    a3_s,
    a3_r,
    out_sem,
):
    T, O, E, span, cap = size["T"], size["O"], size["E"], size["span"], size["cap"]
    share = span * E
    rows = O * share
    half, quarter = rows // 2, rows // 4
    W = nb.shape[2]
    H = gw.shape[0]
    DS = st.shape[1]
    t_half = share // 2
    f32, bf16 = jnp.float32, jnp.bfloat16

    x = lax.axis_index("group")
    c = lax.axis_index("dp")
    t = lax.axis_index("tensor")
    o = x * 2 + c
    odd = lax.rem(t, 2)
    r = (1 - odd) * lax.div(t, 2) + odd * (T - 1 - lax.div(t, 2))

    def at_ring(position):
        p = lax.rem(position, T)
        upper = lax.div(p, T // 2)
        return (1 - upper) * (2 * p) + upper * (2 * (T - 1 - p) + 1)

    nxt, prv = at_ring(r + 1), at_ring(r + T - 1)
    peers = (
        (1 - x, c, {"group": 1 - x}),
        (1 - x, 1 - c, {"group": 1 - x, "dp": 1 - c}),
        (x, 1 - c, {"dp": 1 - c}),
    )
    other_chip, core_peer = {"group": 1 - x}, {"dp": 1 - c}

    def remote(src, dst, send, recv, device):
        return pltpu.make_async_remote_copy(
            src_ref=src, dst_ref=dst, send_sem=send, recv_sem=recv, device_id=device, device_id_type=MESH
        )

    loads = [
        pltpu.make_async_copy(src, dst, load_sem.at[index])
        for index, (src, dst) in enumerate(
            [(student_ref, st), (teacher_ref, th), (project_ref, pw), (gate_ref, gw), (up_ref, uw), (down_ref, dw)]
        )
    ]
    small = [
        pltpu.make_async_copy(src, dst, load_sem.at[len(loads) + index])
        for index, (src, dst) in enumerate(
            [
                (student_gain_in, student_gain_ref),
                (owner_in, owner_ref),
                (ids_in, ids_ref),
                (counts_in, counts_ref),
                (id_weight_in, id_weight_ref),
                (teacher_gain_in, teacher_gain_ref),
            ]
        )
    ]
    for load in (loads[0], *small, *loads[1:]):
        load.start()

    barrier = pltpu.get_barrier_semaphore()
    for _, _, device in peers:
        pl.semaphore_signal(barrier, inc=1, device_id=device, device_id_type=MESH)
    for step in range(1, T):
        pl.semaphore_signal(barrier, inc=1, device_id={"tensor": at_ring(r + step)}, device_id_type=MESH)

    def columns(owner):
        return pl.ds(pl.multiple_of(owner * W, W), W)

    def owner_rows(owner):
        return pl.ds(pl.multiple_of(owner * share, share), share)

    def nx(k):
        return remote(
            nrm.at[:, columns(peers[k][0] * 2 + peers[k][1])],
            nb.at[0, owner_rows(o), :],
            nx_s.at[k],
            nx_r.at[k],
            peers[k][2],
        )

    def raw(k):
        return remote(
            st.at[:, columns(peers[k][0] * 2 + peers[k][1])],
            sb.at[owner_rows(o), :],
            raw_s.at[k],
            raw_r.at[k],
            peers[k][2],
        )

    def extra(k):
        return remote(ext.at[o], ext.at[o], ext_s.at[k], ext_r.at[k], peers[k][2])

    def proj(k):
        return remote(
            pjs.at[:, columns(peers[k][0] * 2 + peers[k][1])],
            pj.at[owner_rows(o), :],
            pj_s.at[k],
            pj_r.at[k],
            peers[k][2],
        )

    out_rows = span * O * cap

    def outgoing(k):
        q = peers[k][0] * 2 + peers[k][1]
        return remote(
            sos.at[pl.ds(pl.multiple_of(q * out_rows, out_rows), out_rows), :],
            so.at[:, columns(o)],
            so_s.at[k],
            so_r.at[k],
            peers[k][2],
        )

    def block_rows(position):
        return pl.ds(pl.multiple_of(at_ring(position) * share, share), share)

    def squares(step):
        return remote(
            sqs.at[block_rows(r + step), :],
            sqr.at[step],
            sq_s.at[step],
            sq_r.at[step],
            {"tensor": at_ring(r + step)},
        )

    def to(d):
        return {"tensor": nxt if d == 0 else prv}

    def part(d, n):
        return pl.ds(d * n, n)

    def ag(d, g):
        return remote(
            nb.at[g - 1, part(d, half), :], nb.at[g, part(d, half), :], ag_s.at[d, g], ag_r.at[d, g], to(d)
        )

    def rs(s, g):
        return remote(
            rss.at[g, part(s, share), :], rsr.at[g, part(s, share), :], rs_s.at[s, g], rs_r.at[s, g], to(s * 2 // O)
        )

    def tr(d, k):
        return remote(
            trs.at[k, part(d, t_half), :], trr.at[k, part(d, t_half), :], tr_s.at[d, k], tr_r.at[d, k], to(d)
        )

    def slot_of(d, s, k):
        return k if (d == 0) == (s < O // 2) else lax.rem(T - k, T)

    def gg(d, s, k):
        return remote(
            ga.at[slot_of(d, s, k - 1), part(s, share), :],
            ga.at[slot_of(d, s, k), part(s, share), :],
            gg_s.at[d * O + s, k],
            gg_r.at[d * O + s, k],
            to(d),
        )

    def gg_order():
        return [(d, s) for s in order for d in (0, 1)]

    def goes_on(d, s):
        return (d == 0) == (s < O // 2)

    order = [s for pair in zip(range(O // 2), range(O // 2, O)) for s in pair]

    def d2(g, m):
        return remote(d2s.at[g, m], d2r.at[g, m], d2_s.at[m, g], d2_r.at[m, g], core_peer)

    def xch(g, m):
        return remote(xs.at[g, m], xr.at[g, m], x_s.at[m, g], x_r.at[m, g], other_chip)

    def act_rows(core, chip):
        return pl.ds(pl.multiple_of((core * 2 + chip) * quarter, quarter), quarter)

    own_act = act_rows(c, x)
    far_act = act_rows(c, 1 - x)

    def a1(g):
        return remote(act.at[g, own_act, :], act.at[g, own_act, :], a1_s.at[g], a1_r.at[g], other_chip)

    def a2(g):
        return remote(act.at[g, own_act, :], act.at[g, own_act, :], a2_s.at[g], a2_r.at[g], core_peer)

    def a3(g):
        return remote(act.at[g, far_act, :], act.at[g, far_act, :], a3_s.at[g], a3_r.at[g], core_peer)

    loads[0].wait()
    small[0].wait()
    wide = st[...].astype(f32)
    rescale = lax.rsqrt(jnp.mean(wide * wide, axis=1, keepdims=True) + EPSILON)
    for j in range(DS // 128):
        lanes = slice(j * 128, (j + 1) * 128)
        nrm[:, lanes] = (wide[:, lanes] * rescale * student_gain_ref[j : j + 1, :]).astype(bf16)
    pl.semaphore_wait(barrier, len(peers) + T - 1)
    for k in range(len(peers)):
        nx(k).start()
    nb[0, owner_rows(o), :] = nrm[:, columns(o)]
    sb[owner_rows(o), :] = st[:, columns(o)]

    def iota(shape, axis):
        return lax.broadcasted_iota(jnp.int32, shape, axis)

    for load in small[1:]:
        load.wait()
    ids = ids_ref[...].astype(f32)
    ids_column = column_of(ids, iota((share, share), 0) == iota((share, share), 1))
    vocabulary = id_weight_ref.shape[1]
    looked = jnp.sum(
        jnp.where(ids_column == iota((share, vocabulary), 1).astype(f32), id_weight_ref[...], 0.0),
        axis=1,
        keepdims=True,
    )
    row_of = iota((share, E), 0)
    counts = column_of(counts_ref[...].astype(f32), lax.rem(row_of, E) == iota((share, E), 1))
    place = (t * span + lax.div(iota((share, 1), 0), E)).astype(f32)
    token_weight = jnp.where(place < counts, looked, 0.0).astype(bf16).astype(f32)
    own_column = column_of(owner_ref[...].astype(f32), iota((E, E), 0) == iota((E, E), 1))
    episode_row, episode_lane = iota((E, 128), 0), lax.rem(iota((E, 128), 1), E)
    own_lane = jnp.sum(jnp.where(episode_row == episode_lane, own_column, 0.0), axis=0, keepdims=True)
    rank = jnp.sum(
        jnp.where((own_column == own_lane) & (episode_row < episode_lane), 1.0, 0.0), axis=0, keepdims=True
    )
    target = own_lane * cap + rank
    ext[o, 0:share, :] = jnp.broadcast_to(token_weight, (share, 128))
    ext[o, share : share + 8, :] = jnp.broadcast_to(target, (8, 128))
    for k in range(len(peers)):
        raw(k).start()
        extra(k).start()

    loads[1].wait()
    wide = th[...].astype(f32)
    scaled[...] = (wide * teacher_gain_ref[...]).astype(bf16)
    sqs[...] = jnp.broadcast_to(jnp.sum(wide * wide, axis=1, keepdims=True), sqs.shape)
    for step in range(1, T):
        squares(step).start()
    loads[2].wait()

    def teacher_tile(offset, n):
        tp[:, pl.ds(offset, n)] = jnp.dot(
            scaled[...], pw[:, pl.ds(offset, n)], preferred_element_type=f32
        ).astype(bf16)

    def forward(k):
        @pl.when(k > 0)
        def _():
            ag(0, k).wait_recv()
            ag(1, k).wait_recv()

        @pl.when(k < T - 1)
        def _():
            ag(0, k + 1).start()
            ag(1, k + 1).start()

    whole = DS // TILE
    early = whole * 2 // 3

    def teacher_loop(index, carry):
        teacher_tile(pl.multiple_of(index * TILE, TILE), TILE)
        return carry

    lax.fori_loop(0, early, teacher_loop, 0)
    for k in range(len(peers)):
        nx(k).wait_recv()
    forward(0)

    def teacher_rest():
        lax.fori_loop(early, whole, teacher_loop, 0)
        if DS > whole * TILE:
            teacher_tile(whole * TILE, DS - whole * TILE)

    trr[0] = jnp.zeros(trr.shape[1:], bf16)
    rsr[0] = jnp.zeros(rsr.shape[1:], bf16)

    def teacher_rows(position, d):
        return pl.ds(pl.multiple_of(at_ring(position) * share + d * t_half, t_half), t_half)

    def teacher_step(k):
        @pl.when(k > 1)
        def _():
            tr(0, k - 1).wait_recv()
            tr(1, k - 1).wait_recv()

        for d in (0, 1):
            position = r + T - k if d == 0 else r + k
            trs[k, part(d, t_half), :] = (
                tp[teacher_rows(position, d), :].astype(f32) + trr[k - 1, part(d, t_half), :].astype(f32)
            ).astype(bf16)
            tr(d, k).start()

    loads[3].wait()
    loads[4].wait()
    loads[5].wait()

    def p1(g):
        away = pl.ds(pl.multiple_of((1 - c) * half, half), half)
        here = pl.ds(pl.multiple_of(c * half, half), half)
        for m, weight in enumerate((gw, uw)):

            def tile(offset, n):
                lhs = jnp.concatenate([nb[g, away, :], nb[g, here, :]], axis=0)
                value = lax.dot_general(
                    lhs, weight[pl.ds(offset, n), :], (((1,), (1,)), ((), ())), preferred_element_type=f32
                )
                d2s[g, m, :, pl.ds(offset, n)] = value[:half].astype(bf16)
                own_part[m, :, pl.ds(offset, n)] = value[half:]

            over_tiles(H, tile)
            d2(g, m).start()

    def p2(g):
        far = pl.ds(pl.multiple_of((1 - x) * quarter, quarter), quarter)
        near = pl.ds(pl.multiple_of(x * quarter, quarter), quarter)
        for m in (0, 1):
            d2(g, m).wait_recv()
            xs[g, m] = (own_part[m, far, :] + d2r[g, m, far, :].astype(f32)).astype(bf16)
            xch(g, m).start()
        for m in (0, 1):
            own_x[g, m] = own_part[m, near, :] + d2r[g, m, near, :].astype(f32)

    def p3(g):
        xch(g, 0).wait_recv()
        xch(g, 1).wait_recv()
        gate = own_x[g, 0] + xr[g, 0].astype(f32)
        up = own_x[g, 1] + xr[g, 1].astype(f32)
        act[g, own_act, :] = (gate / (1.0 + jnp.exp(-gate)) * up).astype(bf16)
        a1(g).start()
        a2(g).start()

    def p4(g):
        a1(g).wait_recv()
        a3(g).start()

    far_hop = T // 2
    act_store = pltpu.make_async_copy(act_t.at[far_hop], act_out, out_sem.at[0])

    def p5(g):
        a2(g).wait_recv()
        a3(g).wait_recv()

        kept = jnp.minimum(g, 1)

        def tile(offset, n):
            bp[kept, :, pl.ds(offset, n)] = jnp.dot(act[g], dw[:, pl.ds(offset, n)], preferred_element_type=f32)

        over_tiles(W, tile)

        @pl.when(g > 0)
        def _():
            for s in order:

                @pl.when(g > 1)
                def _():
                    rs(s, g - 1).wait_recv()

                own = part(s, share)
                rss[g, own, :] = (bp[1, own, :] + rsr[g - 1, own, :].astype(f32)).astype(bf16)
                rs(s, g).start()

        act_t[g] = act[g].T

        @pl.when(g == far_hop)
        def _():
            act_store.start()

    def finish_teacher():
        tr(0, T - 1).wait_recv()
        tr(1, T - 1).wait_recv()
        total = sqs[block_rows(r), :]
        for step in range(1, T):
            squares(step).wait_recv()
            total = total + sqr[step]
        inverse_ref[...] = lax.rsqrt(total * (1.0 / size["teacher_width"]) + EPSILON)
        for d in (0, 1):
            summed = tp[teacher_rows(r, d), :].astype(f32) + trr[T - 1, part(d, t_half), :].astype(f32)
            pjs[part(d, t_half), :] = (summed * inverse_ref[part(d, t_half), 0:1]).astype(bf16)
        for k in range(len(peers)):
            proj(k).start()
        pj[owner_rows(o), :] = pjs[:, columns(o)]

    first = T // 2

    def step(i, carry):
        @pl.when(i < T)
        def _():
            p1(i)

        @pl.when(i + 1 < T)
        def _():
            forward(i + 1)

        @pl.when((i >= 3) & (i < T + 3))
        def _():
            p4(i - 3)

        @pl.when((i >= T - 1) & (i < T + T - 2 - first))
        def _():
            teacher_step(i - (T - 2 - first))

        @pl.when(i == T + T - 2 - first)
        def _():
            finish_teacher()

        @pl.when((i >= 2) & (i < T + 2))
        def _():
            p3(i - 2)

        @pl.when(i < T)
        def _():
            p2(i)

        @pl.when(i < first)
        def _():
            @pl.when(i == 0)
            def _():
                teacher_rest()

            teacher_step(i + 1)

        @pl.when(i >= 3)
        def _():
            p5(i - 3)

        return carry

    lax.fori_loop(0, T + 3, step, 0)

    for k in range(len(peers)):
        raw(k).wait_recv()
        extra(k).wait_recv()
        proj(k).wait_recv()
    for s in order:
        rs(s, T - 1).wait_recv()
        own = slice(s * share, (s + 1) * share)
        predicted = sb[own, :].astype(f32) + (bp[0, own, :] + rsr[T - 1, own, :].astype(f32))
        predb[own, :] = predicted.astype(bf16)
        difference = predicted - pj[own, :].astype(f32)
        ga[0, own, :] = (ext[s, 0:share, 0:1] * difference * size["scale"]).astype(bf16)
        for d in (0, 1):
            gg(d, s, 1).start()

    grad_store = pltpu.make_async_copy(ga.at[far_hop], grad_out, out_sem.at[1])
    pieces = [slice(j, min(j + TAIL, W)) for j in range(0, W, TAIL)]
    sum_stores = [
        pltpu.make_async_copy(acc.at[:, lanes], sum_out.at[:, lanes], out_sem.at[3 + j])
        for j, lanes in enumerate(pieces)
    ]

    lane = iota((1, rows), 1)
    wanted_target = jnp.zeros((1, rows), f32)
    for s in range(O):
        wanted_target = jnp.where(lax.div(lane, share) == s, ext[s, share : share + 1, :], wanted_target)
    picks = O * out_rows
    line = iota((picks, rows), 0)
    place_row = lax.rem(lax.div(line, O * cap), span)
    source_row = lax.rem(lax.div(line, cap), O)
    slot = (lax.div(line, out_rows) * cap + lax.rem(line, cap)).astype(f32)
    lanes = iota((picks, rows), 1)
    chosen = (
        (wanted_target == slot)
        & (lax.div(lanes, share) == source_row)
        & (lax.div(lax.rem(lanes, share), E) == place_row)
    )
    selector = jnp.where(chosen, 1.0, 0.0).astype(bf16)

    def pick_tile(offset, n):
        sos[:, pl.ds(offset, n)] = jnp.dot(
            selector, predb[:, pl.ds(offset, n)], preferred_element_type=f32
        ).astype(bf16)

    over_tiles(W, pick_tile)
    for k in range(len(peers)):
        outgoing(k).start()
    so[:, columns(o)] = sos[pl.ds(pl.multiple_of(o * out_rows, out_rows), out_rows), :]

    def product(k, lanes):
        @pl.when(k == 0)
        def _():
            acc[:, lanes] = jnp.dot(act_t[0], ga[0, :, lanes], preferred_element_type=f32)

        @pl.when(k > 0)
        def _():
            near, back = jnp.maximum(k, 1), T - jnp.maximum(k, 1)
            lhs = jnp.concatenate([act_t[near], act_t[back]], axis=1)
            rhs = jnp.concatenate([ga[near, :, lanes], ga[back, :, lanes]], axis=0)
            acc[:, lanes] += jnp.dot(lhs, rhs, preferred_element_type=f32)

    def gather_step(k, carry):
        steps = gg_order()
        for index, (d, s) in enumerate(steps):
            if goes_on(d, s):
                gg(d, s, k).wait_recv()

                @pl.when(k < far_hop)
                def _():
                    gg(d, s, k + 1).start()
            else:

                @pl.when(k < far_hop)
                def _():
                    gg(d, s, k).wait_recv()

                @pl.when(k < far_hop - 1)
                def _():
                    gg(d, s, k + 1).start()

            for j in range(index * len(pieces) // len(steps), (index + 1) * len(pieces) // len(steps)):
                product(k - 1, pieces[j])

                @pl.when(k == far_hop)
                def _():
                    sum_stores[j].start()

        return carry

    lax.fori_loop(1, far_hop + 1, gather_step, 0)
    grad_store.start()

    for k in range(len(peers)):
        outgoing(k).wait_recv()
    student_store = pltpu.make_async_copy(so, student_out, out_sem.at[2])
    student_store.start()

    def drain(g, carry):
        for copy in (a1, a2, a3):
            copy(g).wait_send()
        for m in (0, 1):
            d2(g, m).wait_send()
            xch(g, m).wait_send()

        @pl.when(g > 0)
        def _():
            squares(g).wait_send()
            for d in (0, 1):
                ag(d, g).wait_send()
                tr(d, g).wait_send()
            for s in range(O):
                rs(s, g).wait_send()

        @pl.when((g > 0) & (g <= far_hop))
        def _():
            for d, s in gg_order():
                if goes_on(d, s):
                    gg(d, s, g).wait_send()
                else:

                    @pl.when(g < far_hop)
                    def _():
                        gg(d, s, g).wait_send()

        return carry

    lax.fori_loop(0, T, drain, 0)
    for k in range(len(peers)):
        nx(k).wait_send()
        raw(k).wait_send()
        extra(k).wait_send()
        proj(k).wait_send()
        outgoing(k).wait_send()
    for copy in (act_store, grad_store, student_store, *sum_stores):
        copy.wait()


def last_terms(
    sum_ref, act_ref, grad_ref, student_ref, out_ref, student_out, total, act, grad, student, small_sem, in_sem, out_sem
):
    height = total.shape[0]
    blocks = [pl.ds(j, min(TAIL, height - j)) for j in range(0, height, TAIL)]
    small = [
        pltpu.make_async_copy(act_ref, act, small_sem.at[0]),
        pltpu.make_async_copy(grad_ref, grad, small_sem.at[1]),
    ]
    student_load = pltpu.make_async_copy(student_ref, student, small_sem.at[2])
    student_store = pltpu.make_async_copy(student, student_out, small_sem.at[3])
    loads = [pltpu.make_async_copy(sum_ref.at[b, :], total.at[b, :], in_sem.at[j]) for j, b in enumerate(blocks)]
    stores = [pltpu.make_async_copy(total.at[b, :], out_ref.at[b, :], out_sem.at[j]) for j, b in enumerate(blocks)]
    for copy in (*small, *loads, student_load):
        copy.start()
    for copy in small:
        copy.wait()
    for b, load, store in zip(blocks, loads, stores):
        term = jnp.dot(act[b, :], grad[...], preferred_element_type=jnp.float32)
        load.wait()
        total[b, :] += term
        store.start()
    student_load.wait()
    student_store.start()
    for copy in (*stores, student_store):
        copy.wait()


def fused(
    teacher_hidden,
    teacher_gain,
    project_weight,
    student_hidden,
    student_gain,
    gate_weight,
    up_weight,
    down_weight,
    owner_map,
    token_ids,
    token_counts,
    id_weight,
):
    f32, bf16 = jnp.float32, jnp.bfloat16
    T, O = lax.axis_size("tensor"), lax.axis_size("group") * lax.axis_size("dp")
    E = token_counts.shape[0]
    span = EP_LEN // T
    share = span * E
    rows = O * share
    half, quarter = rows // 2, rows // 4
    cap = max(2, 2 * E // O)
    local_tokens, F = teacher_hidden.shape
    DS = student_hidden.shape[1]
    W, H = gate_weight.shape
    out_rows = span * O * cap
    size = dict(
        T=T,
        O=O,
        E=E,
        span=span,
        cap=cap,
        teacher_width=F * T,
        scale=1.0 / math.sqrt(EP_LEN * E * O),
    )
    anywhere = pl.BlockSpec(memory_space=pl.ANY)
    DMA = pltpu.SemaphoreType.DMA
    scratch = [
        pltpu.VMEM((local_tokens, F), bf16),
        pltpu.VMEM((local_tokens, F), bf16),
        pltpu.VMEM((F, DS), bf16),
        pltpu.VMEM((local_tokens, DS), bf16),
        pltpu.VMEM((share, DS), bf16),
        pltpu.VMEM((share, DS), bf16),
        pltpu.VMEM((H, W), bf16),
        pltpu.VMEM((H, W), bf16),
        pltpu.VMEM((H, W), bf16),
        pltpu.VMEM((T, rows, W), bf16),
        pltpu.VMEM((2, half, H), f32),
        pltpu.VMEM((T, 2, half, H), bf16),
        pltpu.VMEM((T, 2, half, H), bf16),
        pltpu.VMEM((T, 2, quarter, H), f32),
        pltpu.VMEM((T, 2, quarter, H), bf16),
        pltpu.VMEM((T, 2, quarter, H), bf16),
        pltpu.VMEM((T, rows, H), bf16),
        pltpu.VMEM((2, rows, W), f32),
        pltpu.VMEM((T, rows, W), bf16),
        pltpu.VMEM((T, rows, W), bf16),
        pltpu.VMEM((T, share, DS), bf16),
        pltpu.VMEM((T, share, DS), bf16),
        pltpu.VMEM((local_tokens, 128), f32),
        pltpu.VMEM((T, share, 128), f32),
        pltpu.VMEM((share, 128), f32),
        pltpu.VMEM((share, DS), bf16),
        pltpu.VMEM((rows, W), bf16),
        pltpu.VMEM((rows, W), bf16),
        pltpu.VMEM((O, share + 8, 128), f32),
        pltpu.VMEM((T, rows, W), bf16),
        pltpu.VMEM((T, H, rows), bf16),
        pltpu.VMEM((H, W), f32),
        pltpu.VMEM((rows, W), bf16),
        pltpu.VMEM((O * out_rows, W), bf16),
        pltpu.VMEM((out_rows, DS), bf16),
        pltpu.VMEM((DS // 128, 128), f32),
        pltpu.VMEM((1, E), jnp.int32),
        pltpu.VMEM((1, share), jnp.int32),
        pltpu.VMEM((1, E), jnp.int32),
        pltpu.VMEM((1, id_weight.shape[0]), f32),
        pltpu.VMEM((1, F), f32),
        DMA((12,)),
        *[DMA((3,)) for _ in range(10)],
        *[DMA((T,)) for _ in range(2)],
        *[DMA((2, T)) for _ in range(4)],
        *[DMA((O, T)) for _ in range(2)],
        *[DMA((2 * O, T // 2 + 1)) for _ in range(2)],
        *[DMA((2, T)) for _ in range(4)],
        *[DMA((T,)) for _ in range(6)],
        DMA((3 + pl.cdiv(W, TAIL),)),
    ]
    grads, acts, out, summed = pl.pallas_call(
        functools.partial(fused_kernel, size),
        out_shape=(
            jax.ShapeDtypeStruct((rows, W), bf16),
            jax.ShapeDtypeStruct((H, rows), bf16),
            jax.ShapeDtypeStruct((out_rows, DS), bf16),
            jax.ShapeDtypeStruct((H, W), f32),
        ),
        in_specs=[anywhere] * 12,
        out_specs=(anywhere, anywhere, anywhere, anywhere),
        scratch_shapes=scratch,
        compiler_params=pltpu.CompilerParams(
            collective_id=0, has_side_effects=True, vmem_limit_bytes=63 * 1024 * 1024
        ),
    )(
        teacher_hidden,
        teacher_gain.reshape(1, F),
        project_weight,
        student_hidden,
        student_gain.reshape(DS // 128, 128),
        gate_weight.T,
        up_weight.T,
        down_weight,
        owner_map.reshape(1, E),
        token_ids.reshape(1, share),
        token_counts.reshape(1, E),
        id_weight.reshape(1, -1),
    )
    blocks = pl.cdiv(H, TAIL)
    down_grad, out = pl.pallas_call(
        last_terms,
        out_shape=(jax.ShapeDtypeStruct((H, W), f32), jax.ShapeDtypeStruct((out_rows, DS), bf16)),
        in_specs=[anywhere] * 4,
        out_specs=(anywhere, anywhere),
        scratch_shapes=[
            pltpu.VMEM((H, W), f32),
            pltpu.VMEM((H, rows), bf16),
            pltpu.VMEM((rows, W), bf16),
            pltpu.VMEM((out_rows, DS), bf16),
            DMA((4,)),
            DMA((blocks,)),
            DMA((blocks,)),
        ],
        compiler_params=pltpu.CompilerParams(vmem_limit_bytes=63 * 1024 * 1024),
    )(summed, acts, grads, out)
    return (out.reshape(1, span, O * cap, DS), down_grad.T)


def fits(mesh):
    return mesh.shape["group"] == 2 and mesh.shape["dp"] == 2 and mesh.shape["tensor"] == 8


def solution(mesh):
    in_specs = (
        P(("group", "dp"), "tensor"),
        P("tensor"),
        P("tensor", None),
        P(("group", "dp", "tensor"), None),
        P(),
        P(("group", "dp"), "tensor"),
        P(("group", "dp"), "tensor"),
        P("tensor", ("group", "dp")),
        P(("group", "dp"), None),
        P(("group", "dp", "tensor")),
        P(("group", "dp")),
        P(),
    )
    out_specs = (P(("group", "dp"), "tensor", None, None), P(("group", "dp"), "tensor"))
    body = fused if fits(mesh) else general
    return jax.shard_map(body, mesh=mesh, in_specs=in_specs, out_specs=out_specs, check_vma=False)
```
